256 devices in a mesh: gx: 64 (over x, z_hi, y, core), gy: 4 (over z_lo).
Axes of the slice: x: 4, y: 4, z: 8 (z_hi: 2, z_lo: 4; z = z_hi * 4 + z_lo), core: 2. Of those that a mesh axis runs over, the one named last changes fastest.
Arguments:
- adjoint: float32 [9, 256, 128, 512], P(None, 'gx', 'gy'), may hold values from -6 to 6
- buoyancy: float32 [256, 128, 512], P('gx', 'gy'), may hold values from 0.5 to 2
- lame_lambda: float32 [256, 128, 512], P('gx', 'gy'), may hold values from 0.5 to 2
- shear_mu: float32 [256, 128, 512], P('gx', 'gy'), may hold values from 0.3 to 1.2
- packed: int32 [64, 64, 4, 12, 256], P('gx', None, 'gy'), may hold values from -2147483648 to 2147483646
- scales: float32 [64, 64, 4, 12], P('gx', None, 'gy'), may hold values from 0.005 to 0.05
- perm: int32 [64, 64], P('gx'), may hold values from 0 to 63, each once within a row
Outputs:
- adjoint_out: float32 [9, 256, 128, 512], P(None, 'gx', 'gy')
- gradients: float32 [2, 256, 128, 512], P(None, 'gx', 'gy')
The draws below stay inside these ranges and needn't reach their ends.
Inputs may be any that keep to these rules, and one draw needn't show every extreme that they name: Each row of perm names every number 0 to 63 once. The words of packed are stored inputs and may cross devices as they are, four signed bytes to a word; only values that a program computes travel in float32.
All inputs are finite; a program needn't handle non-finite values.
Results may differ from the reference program's by a relative error of at most 0.0003.
Values sent between devices are 32-bit elements; how exact they have to be, the bound alone decides.
A program may use at most 128 MiB of HBM per device.

```python
import math
import jax
import jax.numpy as jnp
from jax import lax

CX = 4
CY = 32
CZ = 512
STEPS = 2
COMP = 12
OWNERS = 64
SEGW = 256
NX = 256
NY = 128
NZ = 512
N_GY = 4


def place_ends(values, key, low, top_value):
    longest = values.shape.index(max(values.shape))
    spots = []
    for shift in (0, 1):
        where = [jax.random.randint(jax.random.fold_in(key, axis), (), 0, length) for axis, length in enumerate(values.shape)]
        where[longest] = (where[longest] + shift) % values.shape[longest]
        spots.append(tuple(where))
    return values.at[spots[0]].set(low).at[spots[1]].set(top_value)


def steps_of(stream_key, extent, cuts, low, top_value):
    loudness = 1.0
    for position, parts in cuts:
        draws = jax.random.uniform(jax.random.fold_in(jax.random.fold_in(stream_key, 6), position), (parts,), jnp.float32, low / len(cuts), top_value / len(cuts))
        loudness = loudness * jnp.repeat(jnp.exp(draws), extent[position] // parts).reshape((-1,) + (1,) * (len(extent) - 1 - position))
    return loudness


def normal_values(own_key, shape, spread, bound, cuts=(), kind=jnp.bfloat16):
    values = jax.random.normal(own_key, shape, jnp.float32) * spread
    if len(cuts) > 0:
        values = steps_of(own_key, shape, cuts, -0.22, 0.18) * values
    return jnp.clip(values, min=-bound, max=bound).astype(kind)


def setup_inputs(seed: int = 0) -> dict:
    keys = jax.random.split(jax.random.key(seed), 8)
    adjoint = normal_values(keys[0], (9, NX, NY, NZ), 1.0, 6.0, ((1, 64), (2, 4)), jnp.float32)
    buoyancy = jnp.clip(jnp.exp(math.log(2.0) - 1.3862944 * jax.random.uniform(keys[1], (NX, NY, NZ), jnp.float32) ** steps_of(keys[1], (NX, NY, NZ), ((0, 64), (1, 4)), -0.2, 0.2)), 0.5, 2.0)
    lame_lambda = jnp.clip(jnp.exp(math.log(2.0) - 1.3862944 * jax.random.uniform(keys[2], (NX, NY, NZ), jnp.float32) ** steps_of(keys[2], (NX, NY, NZ), ((0, 64), (1, 4)), -0.2, 0.2)), 0.5, 2.0)
    shear_mu = jnp.clip(jnp.exp(math.log(1.2) - 1.3862944 * jax.random.uniform(keys[3], (NX, NY, NZ), jnp.float32) ** steps_of(keys[3], (NX, NY, NZ), ((0, 64), (1, 4)), -0.2, 0.2)), 0.3, 1.2)
    packed = place_ends(jax.random.randint(keys[4], (OWNERS, OWNERS, N_GY, COMP, SEGW), -2147483648, 2147483647), jax.random.fold_in(keys[4], 1), -2147483648, 2147483646).astype(jnp.int32)
    scales = jnp.clip(jnp.exp(math.log(0.05) - 2.3025851 * jax.random.uniform(keys[5], (OWNERS, OWNERS, N_GY, COMP), jnp.float32) ** steps_of(keys[5], (OWNERS, OWNERS, N_GY, COMP), ((0, 64), (2, 4)), -0.2, 0.2)), 0.005, 0.05)
    perm = jax.vmap(lambda own: jax.random.permutation(own, OWNERS))(jax.random.split(keys[6], OWNERS)).reshape((OWNERS, OWNERS)).astype(jnp.int32)
    return dict(adjoint=adjoint, buoyancy=buoyancy, lame_lambda=lame_lambda, shear_mu=shear_mu, packed=packed, scales=scales, perm=perm)


courant = 0.15


def unpack(words):
    low = (words & 255) - 128
    middle = (jnp.right_shift(words, 8) & 255) - 128
    high = (jnp.right_shift(words, 16) & 255) - 128
    topmost = jnp.right_shift(words, 24)
    return jnp.concatenate([low, middle, high, topmost], axis=-1).astype(jnp.float32)


def inverse_order(row):
    count = row.shape[0]
    slots = jnp.arange(count, dtype=jnp.int32)
    hits = (row[None, :] == slots[:, None]).astype(jnp.int32)
    return jnp.sum(hits * slots[None, :], axis=1).astype(jnp.int32)


def forward_field(packed, scales, perm):
    comp = packed.shape[3]
    by_owner = jnp.swapaxes(packed, 0, 1)
    factors = jnp.swapaxes(scales, 0, 1)

    def one_owner(items):
        words, factor, row = items
        blocks = unpack(words) * factor[..., None]
        ordered = jnp.take(blocks, inverse_order(row), axis=0)
        return jnp.transpose(ordered, (2, 1, 0, 3)).reshape(comp, N_GY, CX, CY, CZ)

    whole_field = lax.map(one_owner, (by_owner, factors, perm))
    whole_field = jnp.transpose(whole_field, (1, 0, 3, 2, 4, 5))
    return whole_field.reshape(comp, NX, NY, NZ)


def step_ahead(field, axis):
    count = field.shape[axis]
    widths = [(0, 0)] * field.ndim
    widths[axis] = (0, 1)
    return jnp.pad(lax.slice_in_dim(field, 1, count, axis=axis), widths)


def step_behind(field, axis):
    count = field.shape[axis]
    widths = [(0, 0)] * field.ndim
    widths[axis] = (1, 0)
    return jnp.pad(lax.slice_in_dim(field, 0, count - 1, axis=axis), widths)


def diff_ahead(field, axis):
    return step_ahead(field, axis) - field


def diff_behind(field, axis):
    return field - step_behind(field, axis)


def move_velocity(velocity, stress, buoyancy):
    scaled = courant * buoyancy
    return [
        velocity[0] - scaled * (diff_ahead(stress[0], 0) + diff_behind(stress[3], 1) + diff_behind(stress[4], 2)),
        velocity[1] - scaled * (diff_behind(stress[3], 0) + diff_ahead(stress[1], 1) + diff_behind(stress[5], 2)),
        velocity[2] - scaled * (diff_behind(stress[4], 0) + diff_behind(stress[5], 1) + diff_ahead(stress[2], 2)),
    ]


def strains(velocity):
    return [
        diff_behind(velocity[0], 0),
        diff_behind(velocity[1], 1),
        diff_behind(velocity[2], 2),
        diff_ahead(velocity[0], 1) + diff_ahead(velocity[1], 0),
        diff_ahead(velocity[0], 2) + diff_ahead(velocity[2], 0),
        diff_ahead(velocity[1], 2) + diff_ahead(velocity[2], 1),
    ]


def move_stress(stress, strain, lame_lambda, shear_mu):
    trace = strain[0] + strain[1] + strain[2]
    result = []
    for index in range(3):
        result.append(stress[index] - courant * (lame_lambda * trace + 2.0 * shear_mu * strain[index]))
    for index in range(3, 6):
        result.append(stress[index] - courant * shear_mu * strain[index])
    return result


def reference(adjoint, buoyancy, lame_lambda, shear_mu, packed, scales, perm):
    forward = forward_field(packed, scales, perm)
    velocity = [adjoint[index] for index in range(3)]
    stress = [adjoint[index] for index in range(3, 9)]
    grad_lambda = jnp.zeros(buoyancy.shape, jnp.float32)
    grad_mu = jnp.zeros(buoyancy.shape, jnp.float32)
    for step in range(STEPS):
        velocity = move_velocity(velocity, stress, buoyancy)
        strain = strains(velocity)
        stress = move_stress(stress, strain, lame_lambda, shear_mu)
        stored = [forward[6 * step + index] for index in range(6)]
        trace = strain[0] + strain[1] + strain[2]
        grad_lambda = grad_lambda + trace * (stored[0] + stored[1] + stored[2])
        grad_mu = grad_mu + 2.0 * (strain[0] * stored[0] + strain[1] * stored[1] + strain[2] * stored[2])
        grad_mu = grad_mu + strain[3] * stored[3] + strain[4] * stored[4] + strain[5] * stored[5]
    return jnp.stack(velocity + stress), jnp.stack([grad_lambda, grad_mu])
```

```python
import functools

import jax
import jax.numpy as jnp
from jax import lax
from jax.experimental import pallas as pl
from jax.experimental.pallas import tpu as pltpu
from jax.sharding import PartitionSpec as P

MESH = pl.DeviceIdType.MESH
COURANT = 0.15
VX, VY, VZ, SXX, SYY, SZZ, SXY, SXZ, SYZ = range(9)
NX, NY, NZ = 4, 32, 512
TOP, END = 8, 40
LAST = NX
SCALE_UNIT = 2.0**31


def inverse_order(row):
    count = row.shape[0]
    slots = jnp.arange(count, dtype=jnp.int32)
    hits = (row[None, :] == slots[:, None]).astype(jnp.int32)
    return jnp.sum(hits * slots[None, :], axis=1)


def rows_of(shape):
    return lax.broadcasted_iota(jnp.int32, shape, 0)


def lanes_of(shape):
    return lax.broadcasted_iota(jnp.int32, shape, 1)


def z_ahead(x):
    return jnp.where(lanes_of(x.shape) == NZ - 1, 0.0, pltpu.roll(x, NZ - 1, 1))


def z_behind(x):
    return jnp.where(lanes_of(x.shape) == 0, 0.0, pltpu.roll(x, 1, 1))


def y_ahead(x, following):
    return pltpu.roll(jnp.where(rows_of(x.shape) == 0, following, x), 7, 0)


def y_behind(x, preceding):
    return pltpu.roll(jnp.where(rows_of(x.shape) == 7, preceding, x), 1, 0)


def kernel(
    count, rows_gy,
    adjoint, buoyancy, lame, shear, words, factors, inverse,
    out, gradients,
    field, mat_b, mat_l, mat_m, strain, grad, held, landed,
    to_lo, to_hi, to_south, to_north, to_corner,
    from_lo, from_hi, from_south, from_north, from_corner,
    load_sem, send_sem, recv_sem, halo_send, halo_recv, out_sem,
):
    me, row = lax.axis_index("gx"), lax.axis_index("gy")
    own_x, own_y = pl.ds(1, NX), pl.ds(TOP, NY)
    has_lo, has_hi = me > 0, me < count - 1
    has_south, has_north = row > 0, row < rows_gy - 1

    loads = [
        pltpu.make_async_copy(adjoint, field.at[:, own_x, own_y, :], load_sem.at[0]),
        pltpu.make_async_copy(buoyancy, mat_b, load_sem.at[1]),
        pltpu.make_async_copy(words, held.at[:, pl.ds(0, 24), :], load_sem.at[2]),
        pltpu.make_async_copy(factors, held.at[:, pl.ds(24, 1), :], load_sem.at[3]),
        pltpu.make_async_copy(lame, mat_l, load_sem.at[4]),
        pltpu.make_async_copy(shear, mat_m, load_sem.at[5]),
    ]
    for load in loads:
        load.start()

    def exchange_peer(t):
        far = 1 - t % 2
        u = t // 2 + (1 - far)
        x, z, y, core = me // 16, (me // 8) % 2, (me // 2) % 4, me % 2
        return (
            ((x + u // 8) % 4) * 16 + ((z + far) % 2) * 8 + ((y + (u // 2) % 4) % 4) * 2 + (core + u % 2) % 2
        )

    exists = {
        (-1, 0): has_lo, (1, 0): has_hi, (0, -1): has_south, (0, 1): has_north,
        (-1, -1): has_lo & has_south, (1, 1): has_hi & has_north,
        (1, -1): has_hi & has_south, (-1, 1): has_lo & has_north,
    }

    barrier = pltpu.get_barrier_semaphore()

    def greet(t, _):
        pl.semaphore_signal(barrier, inc=1, device_id={"gx": exchange_peer(t)}, device_id_type=MESH)
        return 0

    lax.fori_loop(0, count - 1, greet, 0)
    expected = jnp.int32(count - 1)
    for (dx, dy), there in exists.items():
        if dy != 0:
            expected = expected + there.astype(jnp.int32)

            @pl.when(there)
            def _():
                pl.semaphore_signal(
                    barrier, inc=1, device_id={"gx": me + dx, "gy": row + dy}, device_id_type=MESH
                )

    for there, ref in ((has_lo, from_lo), (has_hi, from_hi), (has_south, from_south), (has_north, from_north)):

        @pl.when(jnp.logical_not(there))
        def _():
            ref[...] = jnp.zeros(ref.shape, jnp.float32)

    corners = ((-1, -1), (1, 1), (1, -1), (-1, 1))
    for slot, where in enumerate(corners):

        @pl.when(jnp.logical_not(exists[where]))
        def _():
            for step in range(2):
                from_corner[step, slot] = jnp.zeros((2, NZ), jnp.float32)

    def tile(f, layer, k):
        return field[f, layer, pl.ds(TOP + 8 * k, 8), :]

    nothing = jnp.zeros((8, NZ), jnp.float32)

    def stage(step):
        for k in range(NY // 8):
            at = pl.ds(8 * k, 8)
            b = COURANT * mat_b[0, at, :]
            sxy, sxz, syy, syz, szz = (tile(f, 1, k) for f in (SXY, SXZ, SYY, SYZ, SZZ))
            syy_next = tile(SYY, 1, k + 1) if k < NY // 8 - 1 else nothing
            syz_prior = tile(SYZ, 1, k - 1) if k > 0 else nothing
            to_lo[step, 0, at, :] = tile(VY, 1, k) - b * (sxy + y_ahead(syy, syy_next) - syy + syz - z_behind(syz))
            to_lo[step, 1, at, :] = tile(VZ, 1, k) - b * (
                sxz + syz - y_behind(syz, syz_prior) + z_ahead(szz) - szz
            )
            to_lo[step, 2, at, :] = tile(SXX, 1, k)
            b = COURANT * mat_b[NX - 1, at, :]
            sxx, sxy, sxz = (tile(f, LAST, k) for f in (SXX, SXY, SXZ))
            sxy_prior = tile(SXY, LAST, k - 1) if k > 0 else nothing
            to_hi[step, 0, at, :] = tile(VX, LAST, k) - b * (
                sxy - y_behind(sxy, sxy_prior) - sxx + sxz - z_behind(sxz)
            )
            to_hi[step, 1, at, :] = sxy
            to_hi[step, 2, at, :] = sxz
            if step == 0:
                to_lo[0, 3, at, :] = mat_b[0, at, :]
                to_hi[0, 3, at, :] = mat_b[NX - 1, at, :]
        for i in range(NX):
            layer, at = i + 1, pl.ds(0, 8)
            raw = mat_b[i, at, :]
            b = COURANT * raw
            sxx, sxy, sxz, syy, syz, szz = (tile(f, layer, 0) for f in (SXX, SXY, SXZ, SYY, SYZ, SZZ))
            sxx_next = tile(SXX, layer + 1, 0) if i < NX - 1 else nothing
            sxz_prior = tile(SXZ, layer - 1, 0) if i > 0 else nothing
            rx = tile(VX, layer, 0) - b * (sxx_next - sxx + sxy + sxz - z_behind(sxz))
            rz = tile(VZ, layer, 0) - b * (sxz - sxz_prior + syz + z_ahead(szz) - szz)
            for f, value in enumerate((rx, rz, syy, raw)[: 4 if step == 0 else 3]):
                to_south[step, pl.ds(4 * f + i, 1), :] = value[0:1]
            k, at = NY // 8 - 1, pl.ds(NY - 8, 8)
            raw = mat_b[i, at, :]
            b = COURANT * raw
            sxy, syy, syz = (tile(f, layer, k) for f in (SXY, SYY, SYZ))
            sxy_prior = tile(SXY, layer - 1, k) if i > 0 else nothing
            ry = tile(VY, layer, k) - b * (sxy - sxy_prior - syy + syz - z_behind(syz))
            for f, value in enumerate((ry, sxy, syz, raw)[: 4 if step == 0 else 3]):
                to_north[step, pl.ds(4 * f + i, 1), :] = value[7:8]
        k = NY // 8 - 1
        to_corner[step, 0, 0:1] = tile(SXY, LAST, k)[7:8]
        to_corner[step, 1, 0:1] = tile(SXX, 1, 0)[0:1]
        to_corner[step, 1, 1:2] = tile(SYY, 1, 0)[0:1]
        to_corner[step, 2, 0:1] = tile(SYZ, 1, k)[7:8]
        to_corner[step, 3, 0:1] = tile(SXZ, LAST, 0)[0:1]

    def halo_copies(step):
        full = 4 if step == 0 else 3
        faces = [
            (to_lo.at[step, pl.ds(0, full)], from_hi.at[step, pl.ds(0, full)], (-1, 0)),
            (to_hi.at[step, pl.ds(0, full)], from_lo.at[step, pl.ds(0, full)], (1, 0)),
            (to_south.at[step], from_north.at[step], (0, -1)),
            (to_north.at[step], from_south.at[step], (0, 1)),
        ]
        for slot, (dx, dy) in enumerate(corners):
            faces.append((to_corner.at[step, slot], from_corner.at[step, slot], (-dx, -dy)))
        return [
            (
                pltpu.make_async_remote_copy(
                    src_ref=src, dst_ref=dst, send_sem=halo_send.at[step, n], recv_sem=halo_recv.at[step, n],
                    device_id={"gx": me + dx, "gy": row + dy}, device_id_type=MESH,
                ),
                exists[(dx, dy)], exists[(-dx, -dy)],
            )
            for n, (src, dst, (dx, dy)) in enumerate(faces)
        ]

    def send_halo(step):
        for copy, there, _ in halo_copies(step):

            @pl.when(there)
            def _():
                copy.start()

    def take_halo(step):
        for copy, _, comes in halo_copies(step):

            @pl.when(comes)
            def _():
                copy.wait_recv()

    def finish_halo(step):
        sxy_ll = from_corner[step, 0, 0:1]
        sxx_hh, syy_hh = from_corner[step, 1, 0:1], from_corner[step, 1, 1:2]
        syz_hl, sxz_lh = from_corner[step, 2, 0:1], from_corner[step, 3, 0:1]
        for k in range(NY // 8):
            at, framed = pl.ds(8 * k, 8), pl.ds(TOP + 8 * k, 8)
            b = COURANT * from_lo[0, 3, at, :]
            vx = from_lo[step, 0, at, :] - b * tile(SXX, 1, k)
            if k == 0:
                vx = jnp.where(rows_of(vx.shape) == 0, vx + b * sxy_ll, vx)
            field[VX, 0, framed, :] = vx
            field[SXY, 0, framed, :] = from_lo[step, 1, at, :]
            field[SXZ, 0, framed, :] = from_lo[step, 2, at, :]
            b = COURANT * from_hi[0, 3, at, :]
            vy = from_hi[step, 0, at, :] + b * tile(SXY, LAST, k)
            vz = from_hi[step, 1, at, :] + b * tile(SXZ, LAST, k)
            if k == NY // 8 - 1:
                vy = jnp.where(rows_of(vy.shape) == 7, vy - b * syy_hh, vy)
            if k == 0:
                vz = jnp.where(rows_of(vz.shape) == 0, vz + b * syz_hl, vz)
            field[VY, LAST + 1, framed, :] = vy
            field[VZ, LAST + 1, framed, :] = vz
            field[SXX, LAST + 1, framed, :] = from_hi[step, 2, at, :]
        for i in range(NX):
            layer = i + 1
            part, sxy, syz = (from_south[step, pl.ds(4 * f + i, 1), :] for f in range(3))
            b = COURANT * from_south[0, pl.ds(12 + i, 1), :]
            vy = part - b * tile(SYY, layer, 0)[0:1]
            if i == 0:
                vy = vy + b * sxy_ll
            field[VY, layer, pl.ds(TOP - 1, 1), :] = vy
            field[SXY, layer, pl.ds(TOP - 1, 1), :] = sxy
            field[SYZ, layer, pl.ds(TOP - 1, 1), :] = syz
            part_x, part_z, syy = (from_north[step, pl.ds(4 * f + i, 1), :] for f in range(3))
            b = COURANT * from_north[0, pl.ds(12 + i, 1), :]
            vx = part_x + b * tile(SXY, layer, NY // 8 - 1)[7:8]
            vz = part_z + b * tile(SYZ, layer, NY // 8 - 1)[7:8]
            if i == NX - 1:
                vx = vx - b * sxx_hh
            if i == 0:
                vz = vz + b * sxz_lh
            field[VX, layer, pl.ds(END, 1), :] = vx
            field[VZ, layer, pl.ds(END, 1), :] = vz
            field[SYY, layer, pl.ds(END, 1), :] = syy

    def dyn(f, layer, start):
        return field[f, layer, pl.ds(start, 8), :]

    def move_velocity(n, _):
        i, k = n // (NY // 8), n % (NY // 8)
        layer, at = i + 1, pl.multiple_of(TOP + 8 * k, 8)
        before, after = pl.multiple_of(8 * k, 8), pl.multiple_of(TOP + 8 + 8 * k, 8)
        b = COURANT * mat_b[i, pl.ds(pl.multiple_of(8 * k, 8), 8), :]
        sxx, syy, szz, sxy, sxz, syz = (dyn(f, layer, at) for f in (SXX, SYY, SZZ, SXY, SXZ, SYZ))
        dx = dyn(SXX, layer + 1, at) - sxx + sxy - y_behind(sxy, dyn(SXY, layer, before)) + sxz - z_behind(sxz)
        field[VX, layer, pl.ds(at, 8), :] = dyn(VX, layer, at) - b * dx
        dy = sxy - dyn(SXY, layer - 1, at) + y_ahead(syy, dyn(SYY, layer, after)) - syy + syz - z_behind(syz)
        field[VY, layer, pl.ds(at, 8), :] = dyn(VY, layer, at) - b * dy
        dz = sxz - dyn(SXZ, layer - 1, at) + syz - y_behind(syz, dyn(SYZ, layer, before)) + z_ahead(szz) - szz
        field[VZ, layer, pl.ds(at, 8), :] = dyn(VZ, layer, at) - b * dz
        return 0

    def move_stress(step, n, _):
        i, k = n // (NY // 8), n % (NY // 8)
        layer, at = i + 1, pl.multiple_of(TOP + 8 * k, 8)
        before, after = pl.multiple_of(8 * k, 8), pl.multiple_of(TOP + 8 + 8 * k, 8)
        flat = pl.ds(pl.multiple_of(8 * k, 8), 8)
        vx, vy, vz = (dyn(f, layer, at) for f in (VX, VY, VZ))
        exx = vx - dyn(VX, layer - 1, at)
        eyy = vy - y_behind(vy, dyn(VY, layer, before))
        ezz = vz - z_behind(vz)
        exy = y_ahead(vx, dyn(VX, layer, after)) - vx + dyn(VY, layer + 1, at) - vy
        exz = z_ahead(vx) - vx + dyn(VZ, layer + 1, at) - vz
        eyz = z_ahead(vy) - vy + y_ahead(vz, dyn(VZ, layer, after)) - vz
        mu = COURANT * mat_m[i, flat, :]
        both = (COURANT * mat_l[i, flat, :]) * (exx + eyy + ezz)
        for f, e in ((SXX, exx), (SYY, eyy), (SZZ, ezz)):
            field[f, layer, pl.ds(at, 8), :] = dyn(f, layer, at) - (both + 2.0 * mu * e)
        for f, e in ((SXY, exy), (SXZ, exz), (SYZ, eyz)):
            field[f, layer, pl.ds(at, 8), :] = dyn(f, layer, at) - mu * e
        for c, e in enumerate((exx, eyy, ezz, exy, exz, eyz)):
            strain[6 * step + c, i, flat, :] = e
        return 0

    loads[0].wait()
    loads[1].wait()
    stage(0)
    loads[2].wait()
    loads[3].wait()
    pl.semaphore_wait(barrier, expected)
    send_halo(0)

    def exchange(peer):
        return pltpu.make_async_remote_copy(
            src_ref=held.at[peer, pl.ds(0, 25)], dst_ref=landed.at[me, pl.ds(0, 25)],
            send_sem=send_sem.at[peer], recv_sem=recv_sem.at[me],
            device_id={"gx": peer}, device_id_type=MESH,
        )

    def launch(t, _):
        exchange(exchange_peer(t)).start()
        return 0

    lax.fori_loop(0, count - 1, launch, 0)
    landed[me] = held[me]
    loads[4].wait()
    loads[5].wait()

    for step in range(2):
        take_halo(step)
        finish_halo(step)
        lax.fori_loop(0, NX * NY // 8, move_velocity, 0)
        lax.fori_loop(0, NX * NY // 8, functools.partial(move_stress, step), 0)
        if step == 0:
            stage(1)
            send_halo(1)

    store = pltpu.make_async_copy(field.at[:, own_x, own_y, :], out, out_sem.at[0])
    store.start()

    def arrive(t, _):
        other = lax.rem(me + t, count)
        pltpu.make_async_remote_copy(
            src_ref=held.at[other, pl.ds(0, 25)], dst_ref=landed.at[other, pl.ds(0, 25)],
            send_sem=send_sem.at[other], recv_sem=recv_sem.at[other],
            device_id={"gx": other}, device_id_type=MESH,
        ).wait()
        return 0

    lax.fori_loop(1, count, arrive, 0)

    def correlate(n, _):
        i, k = n // (NY // 8), n % (NY // 8)
        flat = pl.ds(pl.multiple_of(8 * k, 8), 8)
        holders = [inverse[i * (NY // 2) + 4 * k + r] for r in range(4)]
        pair = rows_of((8, 128)) // 2
        shift = (rows_of((8, 128)) % 2) * 16

        def gathered(line):
            parts = [jnp.broadcast_to(landed[h, pl.ds(line, 1), :], (8, 128)) for h in holders]
            low = jnp.where(pair == 0, parts[0], parts[1])
            high = jnp.where(pair == 2, parts[2], parts[3])
            return jnp.where(pair < 2, low, high)

        scale_rows = gathered(24).astype(jnp.float32) * (1.0 / SCALE_UNIT)

        def stored(c):
            scale = jnp.broadcast_to(scale_rows[:, c : c + 1], (8, 128))
            halves = [gathered(2 * c + half) ^ jnp.int32(-2147483648) for half in range(2)]
            quarters = []
            for extra in (0, 8):
                for word in halves:
                    byte = jnp.right_shift(word, shift + extra) & 255
                    quarters.append((byte.astype(jnp.float32) - 128.0) * scale)
            return jnp.concatenate(quarters, axis=1)

        for_lambda, for_mu = None, None
        for step in range(2):
            e = [strain[6 * step + c, i, flat, :] for c in range(3)]
            trace = e[0] + e[1] + e[2]
            total, twice = None, None
            for c in range(3):
                f = stored(6 * step + c)
                total = f if total is None else total + f
                twice = e[c] * f if twice is None else twice + e[c] * f
            mu = 2.0 * twice
            for c in range(3, 6):
                mu = mu + strain[6 * step + c, i, flat, :] * stored(6 * step + c)
            for_lambda = trace * total if for_lambda is None else for_lambda + trace * total
            for_mu = mu if for_mu is None else for_mu + mu
        grad[0, i, flat, :] = for_lambda
        grad[1, i, flat, :] = for_mu
        return 0

    lax.fori_loop(0, NX * NY // 8, correlate, 0)
    last = pltpu.make_async_copy(grad, gradients, out_sem.at[1])
    last.start()
    for step in range(2):
        for copy, there, _ in halo_copies(step):

            @pl.when(there)
            def _():
                copy.wait_send()

    store.wait()
    last.wait()


def on_device(adjoint, buoyancy, lame_lambda, shear_mu, packed, scales, perm):
    count, rows_gy = lax.axis_size("gx"), lax.axis_size("gy")
    inverse = inverse_order(perm[0])
    words = packed.reshape(count, 24, 128)
    factors = jnp.round(scales[0, :, 0] * SCALE_UNIT).astype(jnp.int32)
    factors = jnp.pad(factors, ((0, 0), (0, 128 - factors.shape[1])))[:, None, :]
    any_space, smem = pl.BlockSpec(memory_space=pl.ANY), pl.BlockSpec(memory_space=pltpu.SMEM)
    f32, i32 = jnp.float32, jnp.int32
    return pl.pallas_call(
        functools.partial(kernel, count, rows_gy),
        out_shape=(
            jax.ShapeDtypeStruct((9, NX, NY, NZ), f32),
            jax.ShapeDtypeStruct((2, NX, NY, NZ), f32),
        ),
        in_specs=[any_space] * 6 + [smem],
        out_specs=(any_space, any_space),
        scratch_shapes=[
            pltpu.VMEM((9, NX + 2, NY + 16, NZ), f32),
            pltpu.VMEM((NX, NY, NZ), f32),
            pltpu.VMEM((NX, NY, NZ), f32),
            pltpu.VMEM((NX, NY, NZ), f32),
            pltpu.VMEM((12, NX, NY, NZ), f32),
            pltpu.VMEM((2, NX, NY, NZ), f32),
            pltpu.VMEM((64, 32, 128), i32),
            pltpu.VMEM((64, 32, 128), i32),
            pltpu.VMEM((2, 4, NY, NZ), f32),
            pltpu.VMEM((2, 4, NY, NZ), f32),
            pltpu.VMEM((2, 16, NZ), f32),
            pltpu.VMEM((2, 16, NZ), f32),
            pltpu.VMEM((2, 4, 2, NZ), f32),
            pltpu.VMEM((2, 4, NY, NZ), f32),
            pltpu.VMEM((2, 4, NY, NZ), f32),
            pltpu.VMEM((2, 16, NZ), f32),
            pltpu.VMEM((2, 16, NZ), f32),
            pltpu.VMEM((2, 4, 2, NZ), f32),
            pltpu.SemaphoreType.DMA((6,)),
            pltpu.SemaphoreType.DMA((64,)),
            pltpu.SemaphoreType.DMA((64,)),
            pltpu.SemaphoreType.DMA((2, 8)),
            pltpu.SemaphoreType.DMA((2, 8)),
            pltpu.SemaphoreType.DMA((2,)),
        ],
        compiler_params=pltpu.CompilerParams(
            collective_id=0, has_side_effects=True, vmem_limit_bytes=40 * 2**20
        ),
    )(adjoint, buoyancy, lame_lambda, shear_mu, words, factors, inverse)


def solution(mesh):
    return jax.shard_map(
        on_device,
        mesh=mesh,
        in_specs=(
            P(None, "gx", "gy", None),
            P("gx", "gy", None),
            P("gx", "gy", None),
            P("gx", "gy", None),
            P("gx", None, "gy", None, None),
            P("gx", None, "gy", None),
            P("gx", None),
        ),
        out_specs=(P(None, "gx", "gy", None), P(None, "gx", "gy", None)),
        check_vma=False,
    )
```

```python
import functools

import jax
import jax.numpy as jnp
from jax import lax
from jax.experimental import pallas as pl
from jax.experimental.pallas import tpu as pltpu
from jax.sharding import PartitionSpec as P

MESH = pl.DeviceIdType.MESH
COURANT = 0.15
VX, VY, VZ, SXX, SYY, SZZ, SXY, SXZ, SYZ = range(9)
NX, NY, NZ = 4, 32, 512
TOP, END = 8, 40
LAST = NX
SCALE_UNIT = 2.0**31


def rows_of(shape):
    return lax.broadcasted_iota(jnp.int32, shape, 0)


def lanes_of(shape):
    return lax.broadcasted_iota(jnp.int32, shape, 1)


def z_ahead(x):
    return jnp.where(lanes_of(x.shape) == NZ - 1, 0.0, pltpu.roll(x, NZ - 1, 1))


def z_behind(x):
    return jnp.where(lanes_of(x.shape) == 0, 0.0, pltpu.roll(x, 1, 1))


def y_ahead(x, following):
    return pltpu.roll(jnp.where(rows_of(x.shape) == 0, following, x), 7, 0)


def y_behind(x, preceding):
    return pltpu.roll(jnp.where(rows_of(x.shape) == 7, preceding, x), 1, 0)


def kernel(
    count, rows_gy,
    adjoint, buoyancy, lame, shear, words, factors, order,
    out, gradients,
    field, mat_b, mat_l, mat_m, strain, held, landed,
    to_lo, to_hi, to_south, to_north, to_corner,
    from_lo, from_hi, from_south, from_north, from_corner,
    square, factor_rows, order_row, inverse_row, inverse,
    load_sem, send_sem, recv_sem, halo_send, halo_recv, out_sem, ready,
):
    me, row = lax.axis_index("gx"), lax.axis_index("gy")
    own_x, own_y = pl.ds(1, NX), pl.ds(TOP, NY)
    has_lo, has_hi = me > 0, me < count - 1
    has_south, has_north = row > 0, row < rows_gy - 1

    loads = [
        pltpu.make_async_copy(adjoint, field.at[:, own_x, own_y, :], load_sem.at[0]),
        pltpu.make_async_copy(buoyancy, mat_b, load_sem.at[1]),
        pltpu.make_async_copy(words, held.at[:, pl.ds(0, 24), :], load_sem.at[2]),
        pltpu.make_async_copy(factors, factor_rows, load_sem.at[3]),
        pltpu.make_async_copy(lame, mat_l, load_sem.at[4]),
        pltpu.make_async_copy(shear, mat_m, load_sem.at[5]),
        pltpu.make_async_copy(order, order_row, load_sem.at[6]),
    ]
    for load in loads:
        load.start()

    x, z, y, core = me // 16, (me // 8) % 2, (me // 2) % 4, me % 2
    at_x = [((x + d) % 4) * 16 for d in range(4)]
    at_z = [((z + d) % 2) * 8 for d in range(2)]
    at_y = [((y + d) % 4) * 2 for d in range(4)]
    at_core = [(core + d) % 2 for d in range(2)]

    def peer(dx, dz, dy, dcore):
        return at_x[dx] + at_z[dz] + at_y[dy] + at_core[dcore]

    def signal(sem, device):
        pl.semaphore_signal(sem, inc=1, device_id=device, device_id_type=MESH)

    exists = {
        (-1, 0): has_lo, (1, 0): has_hi, (0, -1): has_south, (0, 1): has_north,
        (-1, -1): has_lo & has_south, (1, 1): has_hi & has_north,
        (1, -1): has_hi & has_south, (-1, 1): has_lo & has_north,
    }

    barrier = pltpu.get_barrier_semaphore()

    along_x = [peer(d, 0, 0, 0) for d in (1, 2, 3)]
    along_y = [peer(0, 0, d, 0) for d in (1, 2, 3)]
    across_z, across_core = peer(0, 1, 0, 0), peer(0, 0, 0, 1)
    lines = [across_z] + along_x + along_y + [across_core]
    for other in lines:
        signal(barrier, {"gx": other})
    expected = jnp.int32(len(lines))
    for (dx, dy), there in exists.items():
        expected = expected + there.astype(jnp.int32)

        @pl.when(there)
        def _():
            signal(barrier, {"gx": me + dx, "gy": row + dy})

    for there, ref in ((has_lo, from_lo), (has_hi, from_hi), (has_south, from_south), (has_north, from_north)):

        @pl.when(jnp.logical_not(there))
        def _():
            ref[...] = jnp.zeros(ref.shape, jnp.float32)

    corners = ((-1, -1), (1, 1), (1, -1), (-1, 1))
    for slot, where in enumerate(corners):

        @pl.when(jnp.logical_not(exists[where]))
        def _():
            for step in range(2):
                from_corner[step, slot] = jnp.zeros((2, NZ), jnp.float32)

    def tile(f, layer, k):
        return field[f, layer, pl.ds(TOP + 8 * k, 8), :]

    nothing = jnp.zeros((8, NZ), jnp.float32)

    def stage(step):
        for k in range(NY // 8):
            at = pl.ds(8 * k, 8)
            b = COURANT * mat_b[0, at, :]
            sxy, sxz, syy, syz, szz = (tile(f, 1, k) for f in (SXY, SXZ, SYY, SYZ, SZZ))
            syy_next = tile(SYY, 1, k + 1) if k < NY // 8 - 1 else nothing
            syz_prior = tile(SYZ, 1, k - 1) if k > 0 else nothing
            to_lo[step, 0, at, :] = tile(VY, 1, k) - b * (sxy + y_ahead(syy, syy_next) - syy + syz - z_behind(syz))
            to_lo[step, 1, at, :] = tile(VZ, 1, k) - b * (
                sxz + syz - y_behind(syz, syz_prior) + z_ahead(szz) - szz
            )
            to_lo[step, 2, at, :] = tile(SXX, 1, k)
            b = COURANT * mat_b[NX - 1, at, :]
            sxx, sxy, sxz = (tile(f, LAST, k) for f in (SXX, SXY, SXZ))
            sxy_prior = tile(SXY, LAST, k - 1) if k > 0 else nothing
            to_hi[step, 0, at, :] = tile(VX, LAST, k) - b * (
                sxy - y_behind(sxy, sxy_prior) - sxx + sxz - z_behind(sxz)
            )
            to_hi[step, 1, at, :] = sxy
            to_hi[step, 2, at, :] = sxz
            if step == 0:
                to_lo[0, 3, at, :] = mat_b[0, at, :]
                to_hi[0, 3, at, :] = mat_b[NX - 1, at, :]
        for i in range(NX):
            layer, at = i + 1, pl.ds(0, 8)
            raw = mat_b[i, at, :]
            b = COURANT * raw
            sxx, sxy, sxz, syy, syz, szz = (tile(f, layer, 0) for f in (SXX, SXY, SXZ, SYY, SYZ, SZZ))
            sxx_next = tile(SXX, layer + 1, 0) if i < NX - 1 else nothing
            sxz_prior = tile(SXZ, layer - 1, 0) if i > 0 else nothing
            rx = tile(VX, layer, 0) - b * (sxx_next - sxx + sxy + sxz - z_behind(sxz))
            rz = tile(VZ, layer, 0) - b * (sxz - sxz_prior + syz + z_ahead(szz) - szz)
            for f, value in enumerate((rx, rz, syy, raw)[: 4 if step == 0 else 3]):
                to_south[step, pl.ds(4 * f + i, 1), :] = value[0:1]
            k, at = NY // 8 - 1, pl.ds(NY - 8, 8)
            raw = mat_b[i, at, :]
            b = COURANT * raw
            sxy, syy, syz = (tile(f, layer, k) for f in (SXY, SYY, SYZ))
            sxy_prior = tile(SXY, layer - 1, k) if i > 0 else nothing
            ry = tile(VY, layer, k) - b * (sxy - sxy_prior - syy + syz - z_behind(syz))
            for f, value in enumerate((ry, sxy, syz, raw)[: 4 if step == 0 else 3]):
                to_north[step, pl.ds(4 * f + i, 1), :] = value[7:8]
        k = NY // 8 - 1
        to_corner[step, 0, 0:1] = tile(SXY, LAST, k)[7:8]
        to_corner[step, 1, 0:1] = tile(SXX, 1, 0)[0:1]
        to_corner[step, 1, 1:2] = tile(SYY, 1, 0)[0:1]
        to_corner[step, 2, 0:1] = tile(SYZ, 1, k)[7:8]
        to_corner[step, 3, 0:1] = tile(SXZ, LAST, 0)[0:1]

    def halo_copies(step):
        full = 4 if step == 0 else 3
        faces = [
            (to_lo.at[step, pl.ds(0, full)], from_hi.at[step, pl.ds(0, full)], (-1, 0)),
            (to_hi.at[step, pl.ds(0, full)], from_lo.at[step, pl.ds(0, full)], (1, 0)),
            (to_south.at[step], from_north.at[step], (0, -1)),
            (to_north.at[step], from_south.at[step], (0, 1)),
        ]
        for slot, (dx, dy) in enumerate(corners):
            faces.append((to_corner.at[step, slot], from_corner.at[step, slot], (-dx, -dy)))
        return [
            (
                pltpu.make_async_remote_copy(
                    src_ref=src, dst_ref=dst, send_sem=halo_send.at[step, n], recv_sem=halo_recv.at[step, n],
                    device_id={"gx": me + dx, "gy": row + dy}, device_id_type=MESH,
                ),
                exists[(dx, dy)], exists[(-dx, -dy)],
            )
            for n, (src, dst, (dx, dy)) in enumerate(faces)
        ]

    def send_halo(step):
        for copy, there, _ in halo_copies(step):

            @pl.when(there)
            def _():
                copy.start()

    def take_halo(step):
        for copy, _, comes in halo_copies(step):

            @pl.when(comes)
            def _():
                copy.wait_recv()

    def finish_halo(step):
        sxy_ll = from_corner[step, 0, 0:1]
        sxx_hh, syy_hh = from_corner[step, 1, 0:1], from_corner[step, 1, 1:2]
        syz_hl, sxz_lh = from_corner[step, 2, 0:1], from_corner[step, 3, 0:1]
        for k in range(NY // 8):
            at, framed = pl.ds(8 * k, 8), pl.ds(TOP + 8 * k, 8)
            b = COURANT * from_lo[0, 3, at, :]
            vx = from_lo[step, 0, at, :] - b * tile(SXX, 1, k)
            if k == 0:
                vx = jnp.where(rows_of(vx.shape) == 0, vx + b * sxy_ll, vx)
            field[VX, 0, framed, :] = vx
            field[SXY, 0, framed, :] = from_lo[step, 1, at, :]
            field[SXZ, 0, framed, :] = from_lo[step, 2, at, :]
            b = COURANT * from_hi[0, 3, at, :]
            vy = from_hi[step, 0, at, :] + b * tile(SXY, LAST, k)
            vz = from_hi[step, 1, at, :] + b * tile(SXZ, LAST, k)
            if k == NY // 8 - 1:
                vy = jnp.where(rows_of(vy.shape) == 7, vy - b * syy_hh, vy)
            if k == 0:
                vz = jnp.where(rows_of(vz.shape) == 0, vz + b * syz_hl, vz)
            field[VY, LAST + 1, framed, :] = vy
            field[VZ, LAST + 1, framed, :] = vz
            field[SXX, LAST + 1, framed, :] = from_hi[step, 2, at, :]
        for i in range(NX):
            layer = i + 1
            part, sxy, syz = (from_south[step, pl.ds(4 * f + i, 1), :] for f in range(3))
            b = COURANT * from_south[0, pl.ds(12 + i, 1), :]
            vy = part - b * tile(SYY, layer, 0)[0:1]
            if i == 0:
                vy = vy + b * sxy_ll
            field[VY, layer, pl.ds(TOP - 1, 1), :] = vy
            field[SXY, layer, pl.ds(TOP - 1, 1), :] = sxy
            field[SYZ, layer, pl.ds(TOP - 1, 1), :] = syz
            part_x, part_z, syy = (from_north[step, pl.ds(4 * f + i, 1), :] for f in range(3))
            b = COURANT * from_north[0, pl.ds(12 + i, 1), :]
            vx = part_x + b * tile(SXY, layer, NY // 8 - 1)[7:8]
            vz = part_z + b * tile(SYZ, layer, NY // 8 - 1)[7:8]
            if i == NX - 1:
                vx = vx - b * sxx_hh
            if i == 0:
                vz = vz + b * sxz_lh
            field[VX, layer, pl.ds(END, 1), :] = vx
            field[VZ, layer, pl.ds(END, 1), :] = vz
            field[SYY, layer, pl.ds(END, 1), :] = syy

    def dyn(f, layer, start):
        return field[f, layer, pl.ds(start, 8), :]

    def move_velocity(n, _):
        i, k = n // (NY // 8), n % (NY // 8)
        layer, at = i + 1, pl.multiple_of(TOP + 8 * k, 8)
        before, after = pl.multiple_of(8 * k, 8), pl.multiple_of(TOP + 8 + 8 * k, 8)
        b = COURANT * mat_b[i, pl.ds(pl.multiple_of(8 * k, 8), 8), :]
        sxx, syy, szz, sxy, sxz, syz = (dyn(f, layer, at) for f in (SXX, SYY, SZZ, SXY, SXZ, SYZ))
        dx = dyn(SXX, layer + 1, at) - sxx + sxy - y_behind(sxy, dyn(SXY, layer, before)) + sxz - z_behind(sxz)
        field[VX, layer, pl.ds(at, 8), :] = dyn(VX, layer, at) - b * dx
        dy = sxy - dyn(SXY, layer - 1, at) + y_ahead(syy, dyn(SYY, layer, after)) - syy + syz - z_behind(syz)
        field[VY, layer, pl.ds(at, 8), :] = dyn(VY, layer, at) - b * dy
        dz = sxz - dyn(SXZ, layer - 1, at) + syz - y_behind(syz, dyn(SYZ, layer, before)) + z_ahead(szz) - szz
        field[VZ, layer, pl.ds(at, 8), :] = dyn(VZ, layer, at) - b * dz
        return 0

    def move_stress(step, n, _):
        i, k = n // (NY // 8), n % (NY // 8)
        layer, at = i + 1, pl.multiple_of(TOP + 8 * k, 8)
        before, after = pl.multiple_of(8 * k, 8), pl.multiple_of(TOP + 8 + 8 * k, 8)
        flat = pl.ds(pl.multiple_of(8 * k, 8), 8)
        vx, vy, vz = (dyn(f, layer, at) for f in (VX, VY, VZ))
        exx = vx - dyn(VX, layer - 1, at)
        eyy = vy - y_behind(vy, dyn(VY, layer, before))
        ezz = vz - z_behind(vz)
        exy = y_ahead(vx, dyn(VX, layer, after)) - vx + dyn(VY, layer + 1, at) - vy
        exz = z_ahead(vx) - vx + dyn(VZ, layer + 1, at) - vz
        eyz = z_ahead(vy) - vy + y_ahead(vz, dyn(VZ, layer, after)) - vz
        mu = COURANT * mat_m[i, flat, :]
        both = (COURANT * mat_l[i, flat, :]) * (exx + eyy + ezz)
        for f, e in ((SXX, exx), (SYY, eyy), (SZZ, ezz)):
            field[f, layer, pl.ds(at, 8), :] = dyn(f, layer, at) - (both + 2.0 * mu * e)
        for f, e in ((SXY, exy), (SXZ, exz), (SYZ, eyz)):
            field[f, layer, pl.ds(at, 8), :] = dyn(f, layer, at) - mu * e
        for c, e in enumerate((exx, eyy, ezz, exy, exz, eyz)):
            strain[6 * step + c, i, flat, :] = e
        return 0

    def prepare_blocks():
        loads[3].wait()
        loads[2].wait()
        for c in range(12):
            square[pl.ds(c, 1), 0:64] = factor_rows[c]
        turned = jnp.round(square[...].T * SCALE_UNIT).astype(jnp.int32)
        for owner in range(64):
            held[owner, 24:25, :] = turned[owner : owner + 1]
        places = jnp.broadcast_to(square[16:17, :], (128, 128)).T
        hits = places == lanes_of((128, 128)).astype(jnp.float32)
        found = jnp.sum(jnp.where(hits, rows_of((128, 128)), 0), axis=0, keepdims=True)
        inverse_row[...] = found

    loads[0].wait()
    loads[1].wait()
    stage(0)

    def exchange(other):
        return pltpu.make_async_remote_copy(
            src_ref=held.at[other, pl.ds(0, 25)], dst_ref=landed.at[me, pl.ds(0, 25)],
            send_sem=send_sem.at[other], recv_sem=recv_sem.at[me],
            device_id={"gx": other}, device_id_type=MESH,
        )

    def send_plane(dz, dcore):
        for dx in range(4):
            for dy in range(4):
                if (dx, dz, dy, dcore) != (0, 0, 0, 0):
                    exchange(peer(dx, dz, dy, dcore)).start()

    pl.semaphore_wait(barrier, expected)
    send_halo(0)
    for other in along_x:
        signal(ready.at[0], {"gx": other})
    square[...] = jnp.full((128, 128), 999.0, jnp.float32)
    loads[6].wait()
    square[16:17, 0:64] = order_row[...].astype(jnp.float32)
    prepare_blocks()
    landed[me] = held[me]
    to_smem = pltpu.make_async_copy(inverse_row, inverse, load_sem.at[7])
    to_smem.start()
    pl.semaphore_wait(ready.at[0], 3)
    signal(ready.at[1], {"gx": across_z})
    signal(ready.at[1], {"gx": across_core})
    send_plane(0, 0)
    pl.semaphore_wait(ready.at[1], 2)
    signal(ready.at[2], {"gx": across_core})
    send_plane(1, 0)
    send_plane(0, 1)
    pl.semaphore_wait(ready.at[2], 1)
    send_plane(1, 1)
    loads[4].wait()
    loads[5].wait()

    for step in range(2):
        take_halo(step)
        finish_halo(step)
        lax.fori_loop(0, NX * NY // 8, move_velocity, 0)
        lax.fori_loop(0, NX * NY // 8, functools.partial(move_stress, step), 0)
        if step == 0:
            stage(1)
            send_halo(1)

    store = pltpu.make_async_copy(field.at[:, own_x, own_y, :], out, out_sem.at[0])
    store.start()

    def arrive(t, _):
        other = lax.rem(me + t, count)
        pltpu.make_async_remote_copy(
            src_ref=held.at[other, pl.ds(0, 25)], dst_ref=landed.at[other, pl.ds(0, 25)],
            send_sem=send_sem.at[other], recv_sem=recv_sem.at[other],
            device_id={"gx": other}, device_id_type=MESH,
        ).wait()
        return 0

    lax.fori_loop(1, count, arrive, 0)
    to_smem.wait()

    def correlate(n, _):
        i, k = n // (NY // 8), n % (NY // 8)
        flat = pl.ds(pl.multiple_of(8 * k, 8), 8)
        holders = [jnp.clip(inverse[0, i * (NY // 2) + 4 * k + r], 0, count - 1) for r in range(4)]
        pair = rows_of((8, 128)) // 2
        shift = (rows_of((8, 128)) % 2) * 16

        def gathered(line):
            parts = [jnp.broadcast_to(landed[h, pl.ds(line, 1), :], (8, 128)) for h in holders]
            low = jnp.where(pair == 0, parts[0], parts[1])
            high = jnp.where(pair == 2, parts[2], parts[3])
            return jnp.where(pair < 2, low, high)

        scale_rows = gathered(24).astype(jnp.float32) * (1.0 / SCALE_UNIT)

        def stored(c):
            scale = jnp.broadcast_to(scale_rows[:, c : c + 1], (8, 128))
            halves = [gathered(2 * c + half) ^ jnp.int32(-2147483648) for half in range(2)]
            quarters = []
            for extra in (0, 8):
                for word in halves:
                    byte = jnp.right_shift(word, shift + extra) & 255
                    quarters.append((byte.astype(jnp.float32) - 128.0) * scale)
            return jnp.concatenate(quarters, axis=1)

        for_lambda, for_mu = None, None
        for step in range(2):
            e = [strain[6 * step + c, i, flat, :] for c in range(3)]
            trace = e[0] + e[1] + e[2]
            total, twice = None, None
            for c in range(3):
                f = stored(6 * step + c)
                total = f if total is None else total + f
                twice = e[c] * f if twice is None else twice + e[c] * f
            mu = 2.0 * twice
            for c in range(3, 6):
                mu = mu + strain[6 * step + c, i, flat, :] * stored(6 * step + c)
            for_lambda = trace * total if for_lambda is None else for_lambda + trace * total
            for_mu = mu if for_mu is None else for_mu + mu
        gradients[0, i, flat, :] = for_lambda
        gradients[1, i, flat, :] = for_mu
        return 0

    lax.fori_loop(0, NX * NY // 8, correlate, 0)
    for step in range(2):
        for copy, there, _ in halo_copies(step):

            @pl.when(there)
            def _():
                copy.wait_send()

    store.wait()


def hand_over(state, grad, out, gradients, sem):
    copies = [
        pltpu.make_async_copy(state, out, sem.at[0]),
        pltpu.make_async_copy(grad, gradients, sem.at[1]),
    ]
    for copy in copies:
        copy.start()
    for copy in copies:
        copy.wait()


def on_device(adjoint, buoyancy, lame_lambda, shear_mu, packed, scales, perm):
    count, rows_gy = lax.axis_size("gx"), lax.axis_size("gy")
    words = packed.reshape(count, 24, 128)
    factors = jnp.transpose(scales[0], (2, 1, 0))
    any_space, in_vmem = pl.BlockSpec(memory_space=pl.ANY), pl.BlockSpec(memory_space=pltpu.VMEM)
    f32, i32 = jnp.float32, jnp.int32
    inputs = (adjoint, buoyancy, lame_lambda, shear_mu, words, factors, perm)
    inputs = [pltpu.with_memory_space_constraint(x, pltpu.HBM) for x in inputs]
    state, grad = pl.pallas_call(
        functools.partial(kernel, count, rows_gy),
        out_shape=(
            pltpu.VMEM((9, NX, NY, NZ), f32),
            pltpu.VMEM((2, NX, NY, NZ), f32),
        ),
        in_specs=[any_space] * 7,
        out_specs=(any_space, in_vmem),
        scratch_shapes=[
            pltpu.VMEM((9, NX + 2, NY + 16, NZ), f32),
            pltpu.VMEM((NX, NY, NZ), f32),
            pltpu.VMEM((NX, NY, NZ), f32),
            pltpu.VMEM((NX, NY, NZ), f32),
            pltpu.VMEM((12, NX, NY, NZ), f32),
            pltpu.VMEM((64, 32, 128), i32),
            pltpu.VMEM((64, 32, 128), i32),
            pltpu.VMEM((2, 4, NY, NZ), f32),
            pltpu.VMEM((2, 4, NY, NZ), f32),
            pltpu.VMEM((2, 16, NZ), f32),
            pltpu.VMEM((2, 16, NZ), f32),
            pltpu.VMEM((2, 4, 2, NZ), f32),
            pltpu.VMEM((2, 4, NY, NZ), f32),
            pltpu.VMEM((2, 4, NY, NZ), f32),
            pltpu.VMEM((2, 16, NZ), f32),
            pltpu.VMEM((2, 16, NZ), f32),
            pltpu.VMEM((2, 4, 2, NZ), f32),
            pltpu.VMEM((128, 128), f32),
            pltpu.VMEM((12, 1, 64), f32),
            pltpu.VMEM((1, 64), i32),
            pltpu.VMEM((1, 128), i32),
            pltpu.SMEM((1, 128), i32),
            pltpu.SemaphoreType.DMA((8,)),
            pltpu.SemaphoreType.DMA((64,)),
            pltpu.SemaphoreType.DMA((64,)),
            pltpu.SemaphoreType.DMA((2, 8)),
            pltpu.SemaphoreType.DMA((2, 8)),
            pltpu.SemaphoreType.DMA((2,)),
            pltpu.SemaphoreType.REGULAR((3,)),
        ],
        compiler_params=pltpu.CompilerParams(
            collective_id=0, has_side_effects=True, vmem_limit_bytes=32 * 2**20
        ),
    )(*inputs)
    return pl.pallas_call(
        hand_over,
        out_shape=(
            jax.ShapeDtypeStruct((9, NX, NY, NZ), f32),
            jax.ShapeDtypeStruct((2, NX, NY, NZ), f32),
        ),
        in_specs=[any_space] * 2,
        out_specs=(any_space, any_space),
        scratch_shapes=[pltpu.SemaphoreType.DMA((2,))],
    )(*(pltpu.with_memory_space_constraint(x, pltpu.VMEM) for x in (state, grad)))


def solution(mesh):
    return jax.shard_map(
        on_device,
        mesh=mesh,
        in_specs=(
            P(None, "gx", "gy", None),
            P("gx", "gy", None),
            P("gx", "gy", None),
            P("gx", "gy", None),
            P("gx", None, "gy", None, None),
            P("gx", None, "gy", None),
            P("gx", None),
        ),
        out_specs=(P(None, "gx", "gy", None), P(None, "gx", "gy", None)),
        check_vma=False,
    )
```

```python
import functools

import jax
import jax.numpy as jnp
from jax import lax
from jax.experimental import pallas as pl
from jax.experimental.pallas import tpu as pltpu
from jax.sharding import PartitionSpec as P

MESH = pl.DeviceIdType.MESH
COURANT = 0.15
VX, VY, VZ, SXX, SYY, SZZ, SXY, SXZ, SYZ = range(9)
NX, NY, NZ = 4, 32, 512
TOP, END = 8, 40
LAST = NX
SCALE_UNIT = 2.0**31


def rows_of(shape):
    return lax.broadcasted_iota(jnp.int32, shape, 0)


def lanes_of(shape):
    return lax.broadcasted_iota(jnp.int32, shape, 1)


def z_ahead(x):
    return jnp.where(lanes_of(x.shape) == NZ - 1, 0.0, pltpu.roll(x, NZ - 1, 1))


def z_behind(x):
    return jnp.where(lanes_of(x.shape) == 0, 0.0, pltpu.roll(x, 1, 1))


def y_ahead(x, following):
    return pltpu.roll(jnp.where(rows_of(x.shape) == 0, following, x), 7, 0)


def y_behind(x, preceding):
    return pltpu.roll(jnp.where(rows_of(x.shape) == 7, preceding, x), 1, 0)


def kernel(
    count, rows_gy,
    adjoint, buoyancy, lame, shear, words, factors, order,
    out, gradients,
    field, mat_b, mat_l, mat_m, strain, stored, held, landed,
    to_lo, to_hi, to_south, to_north, to_corner,
    from_lo, from_hi, from_south, from_north, from_corner,
    square, factor_rows, order_row, inverse_row, inverse,
    load_sem, send_sem, recv_sem, halo_send, halo_recv, ready,
):
    me, row = lax.axis_index("gx"), lax.axis_index("gy")
    own_x, own_y = pl.ds(1, NX), pl.ds(TOP, NY)
    has_lo, has_hi = me > 0, me < count - 1
    has_south, has_north = row > 0, row < rows_gy - 1

    loads = [
        pltpu.make_async_copy(adjoint, field.at[:, own_x, own_y, :], load_sem.at[0]),
        pltpu.make_async_copy(buoyancy, mat_b, load_sem.at[1]),
        pltpu.make_async_copy(words, held.at[:, pl.ds(0, 24), :], load_sem.at[2]),
        pltpu.make_async_copy(factors, factor_rows, load_sem.at[3]),
        pltpu.make_async_copy(lame, mat_l, load_sem.at[4]),
        pltpu.make_async_copy(shear, mat_m, load_sem.at[5]),
        pltpu.make_async_copy(order, order_row, load_sem.at[6]),
    ]
    for load in loads:
        load.start()

    x, z, y, core = me // 16, (me // 8) % 2, (me // 2) % 4, me % 2
    at_x = [((x + d) % 4) * 16 for d in range(4)]
    at_z = [((z + d) % 2) * 8 for d in range(2)]
    at_y = [((y + d) % 4) * 2 for d in range(4)]
    at_core = [(core + d) % 2 for d in range(2)]

    def peer(dx, dz, dy, dcore):
        return at_x[dx] + at_z[dz] + at_y[dy] + at_core[dcore]

    def signal(sem, device):
        pl.semaphore_signal(sem, inc=1, device_id=device, device_id_type=MESH)

    exists = {
        (-1, 0): has_lo, (1, 0): has_hi, (0, -1): has_south, (0, 1): has_north,
        (-1, -1): has_lo & has_south, (1, 1): has_hi & has_north,
        (1, -1): has_hi & has_south, (-1, 1): has_lo & has_north,
    }

    barrier = pltpu.get_barrier_semaphore()

    along_x = [peer(d, 0, 0, 0) for d in (1, 2, 3)]
    along_y = [peer(0, 0, d, 0) for d in (1, 2, 3)]
    across_z, across_core = peer(0, 1, 0, 0), peer(0, 0, 0, 1)
    lines = [across_z] + along_x + along_y + [across_core]
    for other in lines:
        signal(barrier, {"gx": other})
    expected = jnp.int32(len(lines))
    for (dx, dy), there in exists.items():
        expected = expected + there.astype(jnp.int32)

        @pl.when(there)
        def _():
            signal(barrier, {"gx": me + dx, "gy": row + dy})

    for there, ref in ((has_lo, from_lo), (has_hi, from_hi), (has_south, from_south), (has_north, from_north)):

        @pl.when(jnp.logical_not(there))
        def _():
            ref[...] = jnp.zeros(ref.shape, jnp.float32)

    corners = ((-1, -1), (1, 1), (1, -1), (-1, 1))
    for slot, where in enumerate(corners):

        @pl.when(jnp.logical_not(exists[where]))
        def _():
            for step in range(2):
                from_corner[step, slot] = jnp.zeros((2, NZ), jnp.float32)

    def tile(f, layer, k):
        return field[f, layer, pl.ds(TOP + 8 * k, 8), :]

    nothing = jnp.zeros((8, NZ), jnp.float32)

    def stage_layers(step):
        for k in range(NY // 8):
            at = pl.ds(8 * k, 8)
            b = COURANT * mat_b[0, at, :]
            sxy, sxz, syy, syz, szz = (tile(f, 1, k) for f in (SXY, SXZ, SYY, SYZ, SZZ))
            syy_next = tile(SYY, 1, k + 1) if k < NY // 8 - 1 else nothing
            syz_prior = tile(SYZ, 1, k - 1) if k > 0 else nothing
            to_lo[step, 0, at, :] = tile(VY, 1, k) - b * (sxy + y_ahead(syy, syy_next) - syy + syz - z_behind(syz))
            to_lo[step, 1, at, :] = tile(VZ, 1, k) - b * (
                sxz + syz - y_behind(syz, syz_prior) + z_ahead(szz) - szz
            )
            to_lo[step, 2, at, :] = tile(SXX, 1, k)
            b = COURANT * mat_b[NX - 1, at, :]
            sxx, sxy, sxz = (tile(f, LAST, k) for f in (SXX, SXY, SXZ))
            sxy_prior = tile(SXY, LAST, k - 1) if k > 0 else nothing
            to_hi[step, 0, at, :] = tile(VX, LAST, k) - b * (
                sxy - y_behind(sxy, sxy_prior) - sxx + sxz - z_behind(sxz)
            )
            to_hi[step, 1, at, :] = sxy
            to_hi[step, 2, at, :] = sxz
            if step == 0:
                to_lo[0, 3, at, :] = mat_b[0, at, :]
                to_hi[0, 3, at, :] = mat_b[NX - 1, at, :]

    def stage_rows(step):
        for i in range(NX):
            layer, at = i + 1, pl.ds(0, 8)
            raw = mat_b[i, at, :]
            b = COURANT * raw
            sxx, sxy, sxz, syy, syz, szz = (tile(f, layer, 0) for f in (SXX, SXY, SXZ, SYY, SYZ, SZZ))
            sxx_next = tile(SXX, layer + 1, 0) if i < NX - 1 else nothing
            sxz_prior = tile(SXZ, layer - 1, 0) if i > 0 else nothing
            rx = tile(VX, layer, 0) - b * (sxx_next - sxx + sxy + sxz - z_behind(sxz))
            rz = tile(VZ, layer, 0) - b * (sxz - sxz_prior + syz + z_ahead(szz) - szz)
            for f, value in enumerate((rx, rz, syy, raw)[: 4 if step == 0 else 3]):
                to_south[step, pl.ds(4 * f + i, 1), :] = value[0:1]
            k, at = NY // 8 - 1, pl.ds(NY - 8, 8)
            raw = mat_b[i, at, :]
            b = COURANT * raw
            sxy, syy, syz = (tile(f, layer, k) for f in (SXY, SYY, SYZ))
            sxy_prior = tile(SXY, layer - 1, k) if i > 0 else nothing
            ry = tile(VY, layer, k) - b * (sxy - sxy_prior - syy + syz - z_behind(syz))
            for f, value in enumerate((ry, sxy, syz, raw)[: 4 if step == 0 else 3]):
                to_north[step, pl.ds(4 * f + i, 1), :] = value[7:8]
        k = NY // 8 - 1
        to_corner[step, 0, 0:1] = tile(SXY, LAST, k)[7:8]
        to_corner[step, 1, 0:1] = tile(SXX, 1, 0)[0:1]
        to_corner[step, 1, 1:2] = tile(SYY, 1, 0)[0:1]
        to_corner[step, 2, 0:1] = tile(SYZ, 1, k)[7:8]
        to_corner[step, 3, 0:1] = tile(SXZ, LAST, 0)[0:1]

    def halo_copies(step, which=slice(None)):
        full = 4 if step == 0 else 3
        faces = [
            (to_lo.at[step, pl.ds(0, full)], from_hi.at[step, pl.ds(0, full)], (-1, 0)),
            (to_hi.at[step, pl.ds(0, full)], from_lo.at[step, pl.ds(0, full)], (1, 0)),
            (to_south.at[step], from_north.at[step], (0, -1)),
            (to_north.at[step], from_south.at[step], (0, 1)),
        ]
        for slot, (dx, dy) in enumerate(corners):
            faces.append((to_corner.at[step, slot], from_corner.at[step, slot], (-dx, -dy)))
        return [
            (
                pltpu.make_async_remote_copy(
                    src_ref=src, dst_ref=dst, send_sem=halo_send.at[step, n], recv_sem=halo_recv.at[step, n],
                    device_id={"gx": me + dx, "gy": row + dy}, device_id_type=MESH,
                ),
                exists[(dx, dy)], exists[(-dx, -dy)],
            )
            for n, (src, dst, (dx, dy)) in list(enumerate(faces))[which]
        ]

    def send_halo(step, which):
        for copy, there, _ in halo_copies(step, which):

            @pl.when(there)
            def _():
                copy.start()

    def take_halo(step):
        for copy, _, comes in halo_copies(step):

            @pl.when(comes)
            def _():
                copy.wait_recv()

    def finish_halo(step):
        sxy_ll = from_corner[step, 0, 0:1]
        sxx_hh, syy_hh = from_corner[step, 1, 0:1], from_corner[step, 1, 1:2]
        syz_hl, sxz_lh = from_corner[step, 2, 0:1], from_corner[step, 3, 0:1]
        for k in range(NY // 8):
            at, framed = pl.ds(8 * k, 8), pl.ds(TOP + 8 * k, 8)
            b = COURANT * from_lo[0, 3, at, :]
            vx = from_lo[step, 0, at, :] - b * tile(SXX, 1, k)
            if k == 0:
                vx = jnp.where(rows_of(vx.shape) == 0, vx + b * sxy_ll, vx)
            field[VX, 0, framed, :] = vx
            b = COURANT * mat_b[0, at, :]
            field[VY, 1, framed, :] = tile(VY, 1, k) + b * from_lo[step, 1, at, :]
            field[VZ, 1, framed, :] = tile(VZ, 1, k) + b * from_lo[step, 2, at, :]
            b = COURANT * from_hi[0, 3, at, :]
            vy = from_hi[step, 0, at, :] + b * tile(SXY, LAST, k)
            vz = from_hi[step, 1, at, :] + b * tile(SXZ, LAST, k)
            if k == NY // 8 - 1:
                vy = jnp.where(rows_of(vy.shape) == 7, vy - b * syy_hh, vy)
            if k == 0:
                vz = jnp.where(rows_of(vz.shape) == 0, vz + b * syz_hl, vz)
            field[VY, LAST + 1, framed, :] = vy
            field[VZ, LAST + 1, framed, :] = vz
            b = COURANT * mat_b[NX - 1, at, :]
            field[VX, LAST, framed, :] = tile(VX, LAST, k) - b * from_hi[step, 2, at, :]
        first, final = pl.ds(TOP, 1), pl.ds(END - 1, 1)
        for i in range(NX):
            layer = i + 1
            part, sxy, syz = (from_south[step, pl.ds(4 * f + i, 1), :] for f in range(3))
            b = COURANT * from_south[0, pl.ds(12 + i, 1), :]
            vy = part - b * field[SYY, layer, first, :]
            if i == 0:
                vy = vy + b * sxy_ll
            field[VY, layer, pl.ds(TOP - 1, 1), :] = vy
            b = COURANT * mat_b[i, 0:1, :]
            field[VX, layer, first, :] = field[VX, layer, first, :] + b * sxy
            field[VZ, layer, first, :] = field[VZ, layer, first, :] + b * syz
            part_x, part_z, syy = (from_north[step, pl.ds(4 * f + i, 1), :] for f in range(3))
            b = COURANT * from_north[0, pl.ds(12 + i, 1), :]
            vx = part_x + b * field[SXY, layer, final, :]
            vz = part_z + b * field[SYZ, layer, final, :]
            if i == NX - 1:
                vx = vx - b * sxx_hh
            if i == 0:
                vz = vz + b * sxz_lh
            field[VX, layer, pl.ds(END, 1), :] = vx
            field[VZ, layer, pl.ds(END, 1), :] = vz
            b = COURANT * mat_b[i, NY - 1 : NY, :]
            field[VY, layer, final, :] = field[VY, layer, final, :] - b * syy

    def dyn(f, layer, start):
        return field[f, layer, pl.ds(start, 8), :]

    def move_velocity(n, _):
        i, k = n // (NY // 8), n % (NY // 8)
        layer, at = i + 1, pl.multiple_of(TOP + 8 * k, 8)
        before, after = pl.multiple_of(8 * k, 8), pl.multiple_of(TOP + 8 + 8 * k, 8)
        b = COURANT * mat_b[i, pl.ds(pl.multiple_of(8 * k, 8), 8), :]
        sxx, syy, szz, sxy, sxz, syz = (dyn(f, layer, at) for f in (SXX, SYY, SZZ, SXY, SXZ, SYZ))
        dx = dyn(SXX, layer + 1, at) - sxx + sxy - y_behind(sxy, dyn(SXY, layer, before)) + sxz - z_behind(sxz)
        field[VX, layer, pl.ds(at, 8), :] = dyn(VX, layer, at) - b * dx
        dy = sxy - dyn(SXY, layer - 1, at) + y_ahead(syy, dyn(SYY, layer, after)) - syy + syz - z_behind(syz)
        field[VY, layer, pl.ds(at, 8), :] = dyn(VY, layer, at) - b * dy
        dz = sxz - dyn(SXZ, layer - 1, at) + syz - y_behind(syz, dyn(SYZ, layer, before)) + z_ahead(szz) - szz
        field[VZ, layer, pl.ds(at, 8), :] = dyn(VZ, layer, at) - b * dz
        return 0

    def move_stress(step, first_layer, stride, n, _):
        i, k = first_layer + stride * (n // (NY // 8)), n % (NY // 8)
        layer, at = i + 1, pl.multiple_of(TOP + 8 * k, 8)
        before, after = pl.multiple_of(8 * k, 8), pl.multiple_of(TOP + 8 + 8 * k, 8)
        flat = pl.ds(pl.multiple_of(8 * k, 8), 8)
        vx, vy, vz = (dyn(f, layer, at) for f in (VX, VY, VZ))
        exx = vx - dyn(VX, layer - 1, at)
        eyy = vy - y_behind(vy, dyn(VY, layer, before))
        ezz = vz - z_behind(vz)
        exy = y_ahead(vx, dyn(VX, layer, after)) - vx + dyn(VY, layer + 1, at) - vy
        exz = z_ahead(vx) - vx + dyn(VZ, layer + 1, at) - vz
        eyz = z_ahead(vy) - vy + y_ahead(vz, dyn(VZ, layer, after)) - vz
        mu = COURANT * mat_m[i, flat, :]
        both = (COURANT * mat_l[i, flat, :]) * (exx + eyy + ezz)
        moved = [dyn(f, layer, at) - (both + 2.0 * mu * e) for f, e in ((SXX, exx), (SYY, eyy), (SZZ, ezz))]
        moved += [dyn(f, layer, at) - mu * e for f, e in ((SXY, exy), (SXZ, exz), (SYZ, eyz))]
        e = (exx, eyy, ezz, exy, exz, eyz)
        if step == 0:
            for f in range(6):
                field[SXX + f, layer, pl.ds(at, 8), :] = moved[f]
                strain[f, i, flat, :] = e[f]
            return 0
        for f, value in enumerate([vx, vy, vz] + moved):
            out[f, i, flat, :] = value
        f = [stored[c, i, flat, :] for c in range(6)]
        gradients[0, i, flat, :] += (exx + eyy + ezz) * (f[0] + f[1] + f[2])
        gradients[1, i, flat, :] += 2.0 * (exx * f[0] + eyy * f[1] + ezz * f[2]) + exy * f[3] + exz * f[4] + eyz * f[5]
        return 0

    blank = jnp.zeros((NY, NZ), jnp.float32)
    field[SXX, LAST + 1, pl.ds(TOP, NY), :] = blank
    field[SXY, 0, pl.ds(TOP, NY), :] = blank
    field[SXZ, 0, pl.ds(TOP, NY), :] = blank
    for layer in range(1, NX + 1):
        field[SYY, layer, pl.ds(END, 8), :] = nothing
        field[SXY, layer, 0:TOP, :] = nothing
        field[SYZ, layer, 0:TOP, :] = nothing

    def prepare_blocks():
        loads[3].wait()
        loads[2].wait()
        for c in range(12):
            square[pl.ds(c, 1), 0:64] = factor_rows[c]
        turned = jnp.round(square[...].T * SCALE_UNIT).astype(jnp.int32)
        for owner in range(64):
            held[owner, 24:25, :] = turned[owner : owner + 1]
        places = jnp.broadcast_to(square[16:17, :], (128, 128)).T
        hits = places == lanes_of((128, 128)).astype(jnp.float32)
        found = jnp.sum(jnp.where(hits, rows_of((128, 128)), 0), axis=0, keepdims=True)
        inverse_row[...] = found

    loads[0].wait()
    loads[1].wait()
    stage_layers(0)
    stage_rows(0)

    def exchange(other):
        return pltpu.make_async_remote_copy(
            src_ref=held.at[other, pl.ds(0, 25)], dst_ref=landed.at[me, pl.ds(0, 25)],
            send_sem=send_sem.at[other], recv_sem=recv_sem.at[me],
            device_id={"gx": other}, device_id_type=MESH,
        )

    def send_plane(dz, dcore):
        for dx in range(4):
            for dy in range(4):
                if (dx, dz, dy, dcore) != (0, 0, 0, 0):
                    exchange(peer(dx, dz, dy, dcore)).start()

    pl.semaphore_wait(barrier, expected)
    send_halo(0, slice(None))
    for other in along_x:
        signal(ready.at[0], {"gx": other})
    square[...] = jnp.full((128, 128), 999.0, jnp.float32)
    loads[6].wait()
    square[16:17, 0:64] = order_row[...].astype(jnp.float32)
    prepare_blocks()
    landed[me] = held[me]
    to_smem = pltpu.make_async_copy(inverse_row, inverse, load_sem.at[7])
    to_smem.start()
    pl.semaphore_wait(ready.at[0], 3)
    signal(ready.at[1], {"gx": across_z})
    signal(ready.at[1], {"gx": across_core})
    send_plane(0, 0)
    pl.semaphore_wait(ready.at[1], 2)
    signal(ready.at[2], {"gx": across_core})
    send_plane(1, 0)
    send_plane(0, 1)
    pl.semaphore_wait(ready.at[2], 1)
    send_plane(1, 1)
    loads[4].wait()
    loads[5].wait()

    def arrive(t, _):
        other = lax.rem(me + t, count)
        pltpu.make_async_remote_copy(
            src_ref=held.at[other, pl.ds(0, 25)], dst_ref=landed.at[other, pl.ds(0, 25)],
            send_sem=send_sem.at[other], recv_sem=recv_sem.at[other],
            device_id={"gx": other}, device_id_type=MESH,
        ).wait()
        return 0

    def correlate(n, _):
        i, k = n // (NY // 8), n % (NY // 8)
        flat = pl.ds(pl.multiple_of(8 * k, 8), 8)
        holders = [jnp.clip(inverse[0, i * (NY // 2) + 4 * k + r], 0, count - 1) for r in range(4)]
        pair = rows_of((8, 128)) // 2
        shift = (rows_of((8, 128)) % 2) * 16

        def gathered(line):
            parts = [jnp.broadcast_to(landed[h, pl.ds(line, 1), :], (8, 128)) for h in holders]
            low = jnp.where(pair == 0, parts[0], parts[1])
            high = jnp.where(pair == 2, parts[2], parts[3])
            return jnp.where(pair < 2, low, high)

        scale_rows = gathered(24).astype(jnp.float32) * (1.0 / SCALE_UNIT)

        def block_values(c):
            scale = jnp.broadcast_to(scale_rows[:, c : c + 1], (8, 128))
            halves = [gathered(2 * c + half) ^ jnp.int32(-2147483648) for half in range(2)]
            quarters = []
            for extra in (0, 8):
                for word in halves:
                    byte = jnp.right_shift(word, shift + extra) & 255
                    quarters.append((byte.astype(jnp.float32) - 128.0) * scale)
            return jnp.concatenate(quarters, axis=1)

        e = [strain[c, i, flat, :] for c in range(6)]
        f = [block_values(c) for c in range(6)]
        gradients[0, i, flat, :] = (e[0] + e[1] + e[2]) * (f[0] + f[1] + f[2])
        gradients[1, i, flat, :] = (
            2.0 * (e[0] * f[0] + e[1] * f[1] + e[2] * f[2]) + e[3] * f[3] + e[4] * f[4] + e[5] * f[5]
        )
        for c in range(6):
            stored[c, i, flat, :] = block_values(6 + c)
        return 0

    tiles = NX * NY // 8
    lax.fori_loop(0, tiles, move_velocity, 0)
    take_halo(0)
    finish_halo(0)
    lax.fori_loop(0, tiles // 2, functools.partial(move_stress, 0, 0, NX - 1), 0)
    stage_layers(1)
    send_halo(1, slice(0, 2))
    lax.fori_loop(0, tiles // 2, functools.partial(move_stress, 0, 1, 1), 0)
    stage_rows(1)
    send_halo(1, slice(2, None))
    lax.fori_loop(0, tiles, move_velocity, 0)
    lax.fori_loop(1, count, arrive, 0)
    to_smem.wait()
    lax.fori_loop(0, tiles, correlate, 0)
    take_halo(1)
    finish_halo(1)
    lax.fori_loop(0, tiles, functools.partial(move_stress, 1, 0, 1), 0)
    for step in range(2):
        for copy, there, _ in halo_copies(step):

            @pl.when(there)
            def _():
                copy.wait_send()


def hand_over(state, grad, out, gradients, sem):
    copies = [
        pltpu.make_async_copy(state, out, sem.at[0]),
        pltpu.make_async_copy(grad, gradients, sem.at[1]),
    ]
    for copy in copies:
        copy.start()
    for copy in copies:
        copy.wait()


def on_device(adjoint, buoyancy, lame_lambda, shear_mu, packed, scales, perm):
    count, rows_gy = lax.axis_size("gx"), lax.axis_size("gy")
    words = packed.reshape(count, 24, 128)
    factors = jnp.transpose(scales[0], (2, 1, 0))
    any_space, in_vmem = pl.BlockSpec(memory_space=pl.ANY), pl.BlockSpec(memory_space=pltpu.VMEM)
    f32, i32 = jnp.float32, jnp.int32
    inputs = (adjoint, buoyancy, lame_lambda, shear_mu, words, factors, perm)
    inputs = [pltpu.with_memory_space_constraint(x, pltpu.HBM) for x in inputs]
    state, grad = pl.pallas_call(
        functools.partial(kernel, count, rows_gy),
        out_shape=(
            pltpu.VMEM((9, NX, NY, NZ), f32),
            pltpu.VMEM((2, NX, NY, NZ), f32),
        ),
        in_specs=[any_space] * 7,
        out_specs=(in_vmem, in_vmem),
        scratch_shapes=[
            pltpu.VMEM((9, NX + 2, NY + 16, NZ), f32),
            pltpu.VMEM((NX, NY, NZ), f32),
            pltpu.VMEM((NX, NY, NZ), f32),
            pltpu.VMEM((NX, NY, NZ), f32),
            pltpu.VMEM((6, NX, NY, NZ), f32),
            pltpu.VMEM((6, NX, NY, NZ), f32),
            pltpu.VMEM((64, 32, 128), i32),
            pltpu.VMEM((64, 32, 128), i32),
            pltpu.VMEM((2, 4, NY, NZ), f32),
            pltpu.VMEM((2, 4, NY, NZ), f32),
            pltpu.VMEM((2, 16, NZ), f32),
            pltpu.VMEM((2, 16, NZ), f32),
            pltpu.VMEM((2, 4, 2, NZ), f32),
            pltpu.VMEM((2, 4, NY, NZ), f32),
            pltpu.VMEM((2, 4, NY, NZ), f32),
            pltpu.VMEM((2, 16, NZ), f32),
            pltpu.VMEM((2, 16, NZ), f32),
            pltpu.VMEM((2, 4, 2, NZ), f32),
            pltpu.VMEM((128, 128), f32),
            pltpu.VMEM((12, 1, 64), f32),
            pltpu.VMEM((1, 64), i32),
            pltpu.VMEM((1, 128), i32),
            pltpu.SMEM((1, 128), i32),
            pltpu.SemaphoreType.DMA((8,)),
            pltpu.SemaphoreType.DMA((64,)),
            pltpu.SemaphoreType.DMA((64,)),
            pltpu.SemaphoreType.DMA((2, 8)),
            pltpu.SemaphoreType.DMA((2, 8)),
            pltpu.SemaphoreType.REGULAR((3,)),
        ],
        compiler_params=pltpu.CompilerParams(
            collective_id=0, has_side_effects=True, vmem_limit_bytes=32 * 2**20
        ),
    )(*inputs)
    return pl.pallas_call(
        hand_over,
        out_shape=(
            jax.ShapeDtypeStruct((9, NX, NY, NZ), f32),
            jax.ShapeDtypeStruct((2, NX, NY, NZ), f32),
        ),
        in_specs=[any_space] * 2,
        out_specs=(any_space, any_space),
        scratch_shapes=[pltpu.SemaphoreType.DMA((2,))],
    )(*(pltpu.with_memory_space_constraint(x, pltpu.VMEM) for x in (state, grad)))


def solution(mesh):
    return jax.shard_map(
        on_device,
        mesh=mesh,
        in_specs=(
            P(None, "gx", "gy", None),
            P("gx", "gy", None),
            P("gx", "gy", None),
            P("gx", "gy", None),
            P("gx", None, "gy", None, None),
            P("gx", None, "gy", None),
            P("gx", None),
        ),
        out_specs=(P(None, "gx", "gy", None), P(None, "gx", "gy", None)),
        check_vma=False,
    )
```

```python
import functools

import jax
import jax.numpy as jnp
from jax import lax
from jax.experimental import pallas as pl
from jax.experimental.pallas import tpu as pltpu
from jax.sharding import PartitionSpec as P

MESH = pl.DeviceIdType.MESH
COURANT = 0.15
VX, VY, VZ, SXX, SYY, SZZ, SXY, SXZ, SYZ = range(9)
NX, NY, NZ = 4, 32, 512
TOP, END = 8, 40
LAST = NX
RELAYED = 2
SCALE_UNIT = 2.0**31


def rows_of(shape):
    return lax.broadcasted_iota(jnp.int32, shape, 0)


def lanes_of(shape):
    return lax.broadcasted_iota(jnp.int32, shape, 1)


def z_ahead(x):
    return jnp.where(lanes_of(x.shape) == NZ - 1, 0.0, pltpu.roll(x, NZ - 1, 1))


def z_behind(x):
    return jnp.where(lanes_of(x.shape) == 0, 0.0, pltpu.roll(x, 1, 1))


def y_ahead(x, following):
    return pltpu.roll(jnp.where(rows_of(x.shape) == 0, following, x), 7, 0)


def y_behind(x, preceding):
    return pltpu.roll(jnp.where(rows_of(x.shape) == 7, preceding, x), 1, 0)


def kernel(
    count, rows_gy,
    adjoint, buoyancy, lame, shear, words, factors, order,
    out, gradients,
    field, mat_b, mat_l, mat_m, strain, stored, held, landed, relay,
    to_lo, to_hi, to_south, to_north, to_corner,
    from_lo, from_hi, from_south, from_north, from_corner,
    square, factor_rows, order_row, inverse_row, inverse,
    load_sem, send_sem, recv_sem, halo_send, halo_recv, relay_send, relay_recv, ready,
):
    me, row = lax.axis_index("gx"), lax.axis_index("gy")
    own_x, own_y = pl.ds(1, NX), pl.ds(TOP, NY)
    has_lo, has_hi = me > 0, me < count - 1
    has_south, has_north = row > 0, row < rows_gy - 1

    loads = [
        pltpu.make_async_copy(adjoint, field.at[:, own_x, own_y, :], load_sem.at[0]),
        pltpu.make_async_copy(buoyancy, mat_b, load_sem.at[1]),
        pltpu.make_async_copy(words, held.at[:, pl.ds(0, 24), :], load_sem.at[2]),
        pltpu.make_async_copy(factors, factor_rows, load_sem.at[3]),
        pltpu.make_async_copy(lame, mat_l, load_sem.at[4]),
        pltpu.make_async_copy(shear, mat_m, load_sem.at[5]),
        pltpu.make_async_copy(order, order_row, load_sem.at[6]),
    ]
    for load in loads:
        load.start()

    x, z, y, core = me // 16, (me // 8) % 2, (me // 2) % 4, me % 2
    at_x = [((x + d) % 4) * 16 for d in range(4)]
    at_z = [((z + d) % 2) * 8 for d in range(2)]
    at_y = [((y + d) % 4) * 2 for d in range(4)]
    at_core = [(core + d) % 2 for d in range(2)]

    def peer(dx, dz, dy, dcore):
        return at_x[dx] + at_z[dz] + at_y[dy] + at_core[dcore]

    def signal(sem, device):
        pl.semaphore_signal(sem, inc=1, device_id=device, device_id_type=MESH)

    exists = {
        (-1, 0): has_lo, (1, 0): has_hi, (0, -1): has_south, (0, 1): has_north,
        (-1, -1): has_lo & has_south, (1, 1): has_hi & has_north,
        (1, -1): has_hi & has_south, (-1, 1): has_lo & has_north,
    }

    barrier = pltpu.get_barrier_semaphore()

    along_x = [peer(d, 0, 0, 0) for d in (1, 2, 3)]
    along_y = [peer(0, 0, d, 0) for d in (1, 2, 3)]
    across_z, across_core = peer(0, 1, 0, 0), peer(0, 0, 0, 1)
    other_half = [peer(dx, 1, dy, dcore) for dcore in range(2) for dx in range(4) for dy in range(4)]
    lines = along_x + along_y + [across_core]
    for other in lines:
        signal(barrier, {"gx": other})

    @pl.when(z == 0)
    def _():
        for other in other_half:
            signal(barrier, {"gx": other})

    expected = len(lines) + len(other_half) * z
    for (dx, dy), there in exists.items():
        expected = expected + there.astype(jnp.int32)

        @pl.when(there)
        def _():
            signal(barrier, {"gx": me + dx, "gy": row + dy})

    for there, ref in ((has_lo, from_lo), (has_hi, from_hi), (has_south, from_south), (has_north, from_north)):

        @pl.when(jnp.logical_not(there))
        def _():
            ref[...] = jnp.zeros(ref.shape, jnp.float32)

    corners = ((-1, -1), (1, 1), (1, -1), (-1, 1))
    for slot, where in enumerate(corners):

        @pl.when(jnp.logical_not(exists[where]))
        def _():
            for step in range(2):
                from_corner[step, slot] = jnp.zeros((2, NZ), jnp.float32)

    def tile(f, layer, k):
        return field[f, layer, pl.ds(TOP + 8 * k, 8), :]

    nothing = jnp.zeros((8, NZ), jnp.float32)

    def stage_layers(step):
        for k in range(NY // 8):
            at = pl.ds(8 * k, 8)
            b = COURANT * mat_b[0, at, :]
            sxy, sxz, syy, syz, szz = (tile(f, 1, k) for f in (SXY, SXZ, SYY, SYZ, SZZ))
            syy_next = tile(SYY, 1, k + 1) if k < NY // 8 - 1 else nothing
            syz_prior = tile(SYZ, 1, k - 1) if k > 0 else nothing
            to_lo[step, 0, at, :] = tile(VY, 1, k) - b * (sxy + y_ahead(syy, syy_next) - syy + syz - z_behind(syz))
            to_lo[step, 1, at, :] = tile(VZ, 1, k) - b * (
                sxz + syz - y_behind(syz, syz_prior) + z_ahead(szz) - szz
            )
            to_lo[step, 2, at, :] = tile(SXX, 1, k)
            b = COURANT * mat_b[NX - 1, at, :]
            sxx, sxy, sxz = (tile(f, LAST, k) for f in (SXX, SXY, SXZ))
            sxy_prior = tile(SXY, LAST, k - 1) if k > 0 else nothing
            to_hi[step, 0, at, :] = tile(VX, LAST, k) - b * (
                sxy - y_behind(sxy, sxy_prior) - sxx + sxz - z_behind(sxz)
            )
            to_hi[step, 1, at, :] = sxy
            to_hi[step, 2, at, :] = sxz
            if step == 0:
                to_lo[0, 3, at, :] = mat_b[0, at, :]
                to_hi[0, 3, at, :] = mat_b[NX - 1, at, :]

    def stage_rows(step):
        for i in range(NX):
            layer, at = i + 1, pl.ds(0, 8)
            raw = mat_b[i, at, :]
            b = COURANT * raw
            sxx, sxy, sxz, syy, syz, szz = (tile(f, layer, 0) for f in (SXX, SXY, SXZ, SYY, SYZ, SZZ))
            sxx_next = tile(SXX, layer + 1, 0) if i < NX - 1 else nothing
            sxz_prior = tile(SXZ, layer - 1, 0) if i > 0 else nothing
            rx = tile(VX, layer, 0) - b * (sxx_next - sxx + sxy + sxz - z_behind(sxz))
            rz = tile(VZ, layer, 0) - b * (sxz - sxz_prior + syz + z_ahead(szz) - szz)
            for f, value in enumerate((rx, rz, syy, raw)[: 4 if step == 0 else 3]):
                to_south[step, pl.ds(4 * f + i, 1), :] = value[0:1]
            k, at = NY // 8 - 1, pl.ds(NY - 8, 8)
            raw = mat_b[i, at, :]
            b = COURANT * raw
            sxy, syy, syz = (tile(f, layer, k) for f in (SXY, SYY, SYZ))
            sxy_prior = tile(SXY, layer - 1, k) if i > 0 else nothing
            ry = tile(VY, layer, k) - b * (sxy - sxy_prior - syy + syz - z_behind(syz))
            for f, value in enumerate((ry, sxy, syz, raw)[: 4 if step == 0 else 3]):
                to_north[step, pl.ds(4 * f + i, 1), :] = value[7:8]
        k = NY // 8 - 1
        to_corner[step, 0, 0:1] = tile(SXY, LAST, k)[7:8]
        to_corner[step, 1, 0:1] = tile(SXX, 1, 0)[0:1]
        to_corner[step, 1, 1:2] = tile(SYY, 1, 0)[0:1]
        to_corner[step, 2, 0:1] = tile(SYZ, 1, k)[7:8]
        to_corner[step, 3, 0:1] = tile(SXZ, LAST, 0)[0:1]

    def halo_copies(step, which=slice(None)):
        full = 4 if step == 0 else 3
        faces = [
            (to_lo.at[step, pl.ds(0, full)], from_hi.at[step, pl.ds(0, full)], (-1, 0)),
            (to_hi.at[step, pl.ds(0, full)], from_lo.at[step, pl.ds(0, full)], (1, 0)),
            (to_south.at[step], from_north.at[step], (0, -1)),
            (to_north.at[step], from_south.at[step], (0, 1)),
        ]
        for slot, (dx, dy) in enumerate(corners):
            faces.append((to_corner.at[step, slot], from_corner.at[step, slot], (-dx, -dy)))
        return [
            (
                pltpu.make_async_remote_copy(
                    src_ref=src, dst_ref=dst, send_sem=halo_send.at[step, n], recv_sem=halo_recv.at[step, n],
                    device_id={"gx": me + dx, "gy": row + dy}, device_id_type=MESH,
                ),
                exists[(dx, dy)], exists[(-dx, -dy)],
            )
            for n, (src, dst, (dx, dy)) in list(enumerate(faces))[which]
        ]

    def send_halo(step, which):
        for copy, there, _ in halo_copies(step, which):

            @pl.when(there)
            def _():
                copy.start()

    def take_halo(step):
        for copy, _, comes in halo_copies(step):

            @pl.when(comes)
            def _():
                copy.wait_recv()

    def finish_halo(step):
        sxy_ll = from_corner[step, 0, 0:1]
        sxx_hh, syy_hh = from_corner[step, 1, 0:1], from_corner[step, 1, 1:2]
        syz_hl, sxz_lh = from_corner[step, 2, 0:1], from_corner[step, 3, 0:1]
        for k in range(NY // 8):
            at, framed = pl.ds(8 * k, 8), pl.ds(TOP + 8 * k, 8)
            b = COURANT * from_lo[0, 3, at, :]
            vx = from_lo[step, 0, at, :] - b * tile(SXX, 1, k)
            if k == 0:
                vx = jnp.where(rows_of(vx.shape) == 0, vx + b * sxy_ll, vx)
            field[VX, 0, framed, :] = vx
            b = COURANT * mat_b[0, at, :]
            field[VY, 1, framed, :] = tile(VY, 1, k) + b * from_lo[step, 1, at, :]
            field[VZ, 1, framed, :] = tile(VZ, 1, k) + b * from_lo[step, 2, at, :]
            b = COURANT * from_hi[0, 3, at, :]
            vy = from_hi[step, 0, at, :] + b * tile(SXY, LAST, k)
            vz = from_hi[step, 1, at, :] + b * tile(SXZ, LAST, k)
            if k == NY // 8 - 1:
                vy = jnp.where(rows_of(vy.shape) == 7, vy - b * syy_hh, vy)
            if k == 0:
                vz = jnp.where(rows_of(vz.shape) == 0, vz + b * syz_hl, vz)
            field[VY, LAST + 1, framed, :] = vy
            field[VZ, LAST + 1, framed, :] = vz
            b = COURANT * mat_b[NX - 1, at, :]
            field[VX, LAST, framed, :] = tile(VX, LAST, k) - b * from_hi[step, 2, at, :]
        first, final = pl.ds(TOP, 1), pl.ds(END - 1, 1)
        for i in range(NX):
            layer = i + 1
            part, sxy, syz = (from_south[step, pl.ds(4 * f + i, 1), :] for f in range(3))
            b = COURANT * from_south[0, pl.ds(12 + i, 1), :]
            vy = part - b * field[SYY, layer, first, :]
            if i == 0:
                vy = vy + b * sxy_ll
            field[VY, layer, pl.ds(TOP - 1, 1), :] = vy
            b = COURANT * mat_b[i, 0:1, :]
            field[VX, layer, first, :] = field[VX, layer, first, :] + b * sxy
            field[VZ, layer, first, :] = field[VZ, layer, first, :] + b * syz
            part_x, part_z, syy = (from_north[step, pl.ds(4 * f + i, 1), :] for f in range(3))
            b = COURANT * from_north[0, pl.ds(12 + i, 1), :]
            vx = part_x + b * field[SXY, layer, final, :]
            vz = part_z + b * field[SYZ, layer, final, :]
            if i == NX - 1:
                vx = vx - b * sxx_hh
            if i == 0:
                vz = vz + b * sxz_lh
            field[VX, layer, pl.ds(END, 1), :] = vx
            field[VZ, layer, pl.ds(END, 1), :] = vz
            b = COURANT * mat_b[i, NY - 1 : NY, :]
            field[VY, layer, final, :] = field[VY, layer, final, :] - b * syy

    def dyn(f, layer, start):
        return field[f, layer, pl.ds(start, 8), :]

    def move_velocity(n, _):
        i, k = n // (NY // 8), n % (NY // 8)
        layer, at = i + 1, pl.multiple_of(TOP + 8 * k, 8)
        before, after = pl.multiple_of(8 * k, 8), pl.multiple_of(TOP + 8 + 8 * k, 8)
        b = COURANT * mat_b[i, pl.ds(pl.multiple_of(8 * k, 8), 8), :]
        sxx, syy, szz, sxy, sxz, syz = (dyn(f, layer, at) for f in (SXX, SYY, SZZ, SXY, SXZ, SYZ))
        dx = dyn(SXX, layer + 1, at) - sxx + sxy - y_behind(sxy, dyn(SXY, layer, before)) + sxz - z_behind(sxz)
        field[VX, layer, pl.ds(at, 8), :] = dyn(VX, layer, at) - b * dx
        dy = sxy - dyn(SXY, layer - 1, at) + y_ahead(syy, dyn(SYY, layer, after)) - syy + syz - z_behind(syz)
        field[VY, layer, pl.ds(at, 8), :] = dyn(VY, layer, at) - b * dy
        dz = sxz - dyn(SXZ, layer - 1, at) + syz - y_behind(syz, dyn(SYZ, layer, before)) + z_ahead(szz) - szz
        field[VZ, layer, pl.ds(at, 8), :] = dyn(VZ, layer, at) - b * dz
        return 0

    def move_stress(step, first_layer, stride, n, _):
        i, k = first_layer + stride * (n // (NY // 8)), n % (NY // 8)
        layer, at = i + 1, pl.multiple_of(TOP + 8 * k, 8)
        before, after = pl.multiple_of(8 * k, 8), pl.multiple_of(TOP + 8 + 8 * k, 8)
        flat = pl.ds(pl.multiple_of(8 * k, 8), 8)
        vx, vy, vz = (dyn(f, layer, at) for f in (VX, VY, VZ))
        exx = vx - dyn(VX, layer - 1, at)
        eyy = vy - y_behind(vy, dyn(VY, layer, before))
        ezz = vz - z_behind(vz)
        exy = y_ahead(vx, dyn(VX, layer, after)) - vx + dyn(VY, layer + 1, at) - vy
        exz = z_ahead(vx) - vx + dyn(VZ, layer + 1, at) - vz
        eyz = z_ahead(vy) - vy + y_ahead(vz, dyn(VZ, layer, after)) - vz
        mu = COURANT * mat_m[i, flat, :]
        both = (COURANT * mat_l[i, flat, :]) * (exx + eyy + ezz)
        moved = [dyn(f, layer, at) - (both + 2.0 * mu * e) for f, e in ((SXX, exx), (SYY, eyy), (SZZ, ezz))]
        moved += [dyn(f, layer, at) - mu * e for f, e in ((SXY, exy), (SXZ, exz), (SYZ, eyz))]
        e = (exx, eyy, ezz, exy, exz, eyz)
        if step == 0:
            for f in range(6):
                field[SXX + f, layer, pl.ds(at, 8), :] = moved[f]
                strain[f, i, flat, :] = e[f]
            return 0
        for f, value in enumerate([vx, vy, vz] + moved):
            out[f, i, flat, :] = value
        f = [stored[c, i, flat, :] for c in range(6)]
        gradients[0, i, flat, :] += (exx + eyy + ezz) * (f[0] + f[1] + f[2])
        gradients[1, i, flat, :] += 2.0 * (exx * f[0] + eyy * f[1] + ezz * f[2]) + exy * f[3] + exz * f[4] + eyz * f[5]
        return 0

    blank = jnp.zeros((NY, NZ), jnp.float32)
    field[SXX, LAST + 1, pl.ds(TOP, NY), :] = blank
    field[SXY, 0, pl.ds(TOP, NY), :] = blank
    field[SXZ, 0, pl.ds(TOP, NY), :] = blank
    for layer in range(1, NX + 1):
        field[SYY, layer, pl.ds(END, 8), :] = nothing
        field[SXY, layer, 0:TOP, :] = nothing
        field[SYZ, layer, 0:TOP, :] = nothing

    def prepare_blocks():
        loads[3].wait()
        loads[2].wait()
        for c in range(12):
            square[pl.ds(c, 1), 0:64] = factor_rows[c]
        turned = jnp.round(square[...].T * SCALE_UNIT).astype(jnp.int32)
        for owner in range(64):
            held[owner, 24:25, :] = turned[owner : owner + 1]
        places = jnp.broadcast_to(square[16:17, :], (128, 128)).T
        hits = places == lanes_of((128, 128)).astype(jnp.float32)
        found = jnp.sum(jnp.where(hits, rows_of((128, 128)), 0), axis=0, keepdims=True)
        inverse_row[...] = found

    loads[0].wait()
    loads[1].wait()
    stage_layers(0)
    stage_rows(0)

    def exchange(other):
        return pltpu.make_async_remote_copy(
            src_ref=held.at[other, pl.ds(0, 25)], dst_ref=landed.at[me, pl.ds(0, 25)],
            send_sem=send_sem, recv_sem=recv_sem,
            device_id={"gx": other}, device_id_type=MESH,
        )

    def blocks_of(ref, sem, number):
        some = ref.at[pl.ds(0, number), pl.ds(0, 25)]
        return pltpu.make_async_copy(some, some, sem)

    def send_near(dcore):
        for dx in range(4):
            for dy in range(4):
                if (dx, dy, dcore) != (0, 0, 0):
                    exchange(peer(dx, 0, dy, dcore)).start()

    edge = (y == 0) | (y == 3)

    def send_far(dcore):
        for dx in range(4):
            if dx == RELAYED:
                continue
            for dy in range(4):
                exchange(peer(dx, 1, dy, dcore)).start()

    def send_far_middle(dcore):
        for dy in range(4):
            exchange(peer(RELAYED, 1, dy, dcore)).start()

    def relayed_owner(n):
        return at_x[RELAYED] + at_z[1] + n

    def to_relay(n):
        owner = relayed_owner(n)
        return pltpu.make_async_remote_copy(
            src_ref=held.at[owner, pl.ds(0, 25)], dst_ref=relay.at[n, pl.ds(0, 25)],
            send_sem=send_sem, recv_sem=relay_recv,
            device_id={"gx": at_x[0] + at_z[0] + (1 + y // 3) * 2 + core}, device_id_type=MESH,
        )

    def from_relay(n):
        holder = at_x[0] + at_z[0] + (y - 1) * 3 * 2 + core
        return pltpu.make_async_remote_copy(
            src_ref=relay.at[n, pl.ds(0, 25)], dst_ref=landed.at[holder, pl.ds(0, 25)],
            send_sem=relay_send, recv_sem=recv_sem,
            device_id={"gx": relayed_owner(n)}, device_id_type=MESH,
        )

    pl.semaphore_wait(barrier, expected)
    send_halo(0, slice(None))
    for other in along_x:
        signal(ready.at[0], {"gx": other})
    square[...] = jnp.full((128, 128), 999.0, jnp.float32)
    loads[6].wait()
    square[16:17, 0:64] = order_row[...].astype(jnp.float32)
    prepare_blocks()

    @pl.when(edge)
    def _():
        for n in range(8):
            to_relay(n).start()

    @pl.when((z == 1) & jnp.logical_not(edge))
    def _():
        for dcore in range(2):
            send_far(dcore)
            send_far_middle(dcore)

    landed[me] = held[me]
    to_smem = pltpu.make_async_copy(inverse_row, inverse, load_sem.at[7])
    to_smem.start()
    pl.semaphore_wait(ready.at[0], 3)
    signal(ready.at[1], {"gx": across_core})

    @pl.when(z == 1)
    def _():
        signal(ready.at[2], {"gx": across_z})

    pl.semaphore_wait(ready.at[1], 1)

    @pl.when((z == 1) & edge)
    def _():
        send_far(0)

    @pl.when(z == 0)
    def _():
        pl.semaphore_wait(ready.at[2], 1)
        signal(ready.at[3], {"gx": across_core})
        send_far(0)
        pl.semaphore_wait(ready.at[3], 1)

    @pl.when((z == 0) & jnp.logical_not(edge))
    def _():
        send_far(1)

    @pl.when((z == 0) & jnp.logical_not(edge))
    def _():
        send_far_middle(0)
        send_far_middle(1)

    @pl.when(jnp.logical_not(edge))
    def _():
        blocks_of(relay, relay_recv, 8).wait()
        for n in range(8):
            from_relay(n).start()

    send_near(0)
    send_near(1)
    loads[4].wait()
    loads[5].wait()

    def correlate(n, _):
        i, k = n // (NY // 8), n % (NY // 8)
        flat = pl.ds(pl.multiple_of(8 * k, 8), 8)
        holders = [jnp.clip(inverse[0, i * (NY // 2) + 4 * k + r], 0, count - 1) for r in range(4)]
        pair = rows_of((8, 128)) // 2
        shift = (rows_of((8, 128)) % 2) * 16

        def gathered(line):
            parts = [jnp.broadcast_to(landed[h, pl.ds(line, 1), :], (8, 128)) for h in holders]
            low = jnp.where(pair == 0, parts[0], parts[1])
            high = jnp.where(pair == 2, parts[2], parts[3])
            return jnp.where(pair < 2, low, high)

        scale_rows = gathered(24).astype(jnp.float32) * (1.0 / SCALE_UNIT)

        def block_values(c):
            scale = jnp.broadcast_to(scale_rows[:, c : c + 1], (8, 128))
            halves = [gathered(2 * c + half) ^ jnp.int32(-2147483648) for half in range(2)]
            quarters = []
            for extra in (0, 8):
                for word in halves:
                    byte = jnp.right_shift(word, shift + extra) & 255
                    quarters.append((byte.astype(jnp.float32) - 128.0) * scale)
            return jnp.concatenate(quarters, axis=1)

        e = [strain[c, i, flat, :] for c in range(6)]
        f = [block_values(c) for c in range(6)]
        gradients[0, i, flat, :] = (e[0] + e[1] + e[2]) * (f[0] + f[1] + f[2])
        gradients[1, i, flat, :] = (
            2.0 * (e[0] * f[0] + e[1] * f[1] + e[2] * f[2]) + e[3] * f[3] + e[4] * f[4] + e[5] * f[5]
        )
        for c in range(6):
            stored[c, i, flat, :] = block_values(6 + c)
        return 0

    tiles = NX * NY // 8
    lax.fori_loop(0, tiles, move_velocity, 0, unroll=2)
    take_halo(0)

    @pl.when(edge)
    def _():
        send_far(1)

    finish_halo(0)
    lax.fori_loop(0, tiles // 2, functools.partial(move_stress, 0, 0, NX - 1), 0, unroll=2)
    stage_layers(1)
    send_halo(1, slice(0, 2))
    lax.fori_loop(0, tiles // 2, functools.partial(move_stress, 0, 1, 1), 0, unroll=2)
    stage_rows(1)
    send_halo(1, slice(2, None))
    lax.fori_loop(0, tiles, move_velocity, 0, unroll=2)
    blocks_of(landed, recv_sem, count - 1).wait()
    to_smem.wait()
    lax.fori_loop(0, tiles, correlate, 0, unroll=2)
    take_halo(1)
    finish_halo(1)
    lax.fori_loop(0, tiles, functools.partial(move_stress, 1, 0, 1), 0, unroll=2)
    for step in range(2):
        for copy, there, _ in halo_copies(step):

            @pl.when(there)
            def _():
                copy.wait_send()

    @pl.when(jnp.logical_not(edge))
    def _():
        blocks_of(relay, relay_send, 8).wait()

    blocks_of(held, send_sem, count - 1).wait()


def hand_over(state, grad, out, gradients, sem):
    copies = [pltpu.make_async_copy(state.at[f], out.at[f], sem.at[f]) for f in range(9)]
    copies += [pltpu.make_async_copy(grad.at[f], gradients.at[f], sem.at[9 + f]) for f in range(2)]
    for copy in copies:
        copy.start()
    for copy in copies:
        copy.wait()


def on_device(adjoint, buoyancy, lame_lambda, shear_mu, packed, scales, perm):
    count, rows_gy = lax.axis_size("gx"), lax.axis_size("gy")
    words = packed.reshape(count, 24, 128)
    factors = jnp.transpose(scales[0], (2, 1, 0))
    any_space, in_vmem = pl.BlockSpec(memory_space=pl.ANY), pl.BlockSpec(memory_space=pltpu.VMEM)
    f32, i32 = jnp.float32, jnp.int32
    inputs = (adjoint, buoyancy, lame_lambda, shear_mu, words, factors, perm)
    inputs = [pltpu.with_memory_space_constraint(x, pltpu.HBM) for x in inputs]
    state, grad = pl.pallas_call(
        functools.partial(kernel, count, rows_gy),
        out_shape=(
            pltpu.VMEM((9, NX, NY, NZ), f32),
            pltpu.VMEM((2, NX, NY, NZ), f32),
        ),
        in_specs=[any_space] * 7,
        out_specs=(in_vmem, in_vmem),
        scratch_shapes=[
            pltpu.VMEM((9, NX + 2, NY + 16, NZ), f32),
            pltpu.VMEM((NX, NY, NZ), f32),
            pltpu.VMEM((NX, NY, NZ), f32),
            pltpu.VMEM((NX, NY, NZ), f32),
            pltpu.VMEM((6, NX, NY, NZ), f32),
            pltpu.VMEM((6, NX, NY, NZ), f32),
            pltpu.VMEM((64, 32, 128), i32),
            pltpu.VMEM((64, 32, 128), i32),
            pltpu.VMEM((8, 32, 128), i32),
            pltpu.VMEM((2, 4, NY, NZ), f32),
            pltpu.VMEM((2, 4, NY, NZ), f32),
            pltpu.VMEM((2, 16, NZ), f32),
            pltpu.VMEM((2, 16, NZ), f32),
            pltpu.VMEM((2, 4, 2, NZ), f32),
            pltpu.VMEM((2, 4, NY, NZ), f32),
            pltpu.VMEM((2, 4, NY, NZ), f32),
            pltpu.VMEM((2, 16, NZ), f32),
            pltpu.VMEM((2, 16, NZ), f32),
            pltpu.VMEM((2, 4, 2, NZ), f32),
            pltpu.VMEM((128, 128), f32),
            pltpu.VMEM((12, 1, 64), f32),
            pltpu.VMEM((1, 64), i32),
            pltpu.VMEM((1, 128), i32),
            pltpu.SMEM((1, 128), i32),
            pltpu.SemaphoreType.DMA((8,)),
            pltpu.SemaphoreType.DMA,
            pltpu.SemaphoreType.DMA,
            pltpu.SemaphoreType.DMA((2, 8)),
            pltpu.SemaphoreType.DMA((2, 8)),
            pltpu.SemaphoreType.DMA,
            pltpu.SemaphoreType.DMA,
            pltpu.SemaphoreType.REGULAR((4,)),
        ],
        compiler_params=pltpu.CompilerParams(
            collective_id=0, has_side_effects=True, vmem_limit_bytes=32 * 2**20
        ),
    )(*inputs)
    return pl.pallas_call(
        hand_over,
        out_shape=(
            jax.ShapeDtypeStruct((9, NX, NY, NZ), f32),
            jax.ShapeDtypeStruct((2, NX, NY, NZ), f32),
        ),
        in_specs=[any_space] * 2,
        out_specs=(any_space, any_space),
        scratch_shapes=[pltpu.SemaphoreType.DMA((11,))],
    )(*(pltpu.with_memory_space_constraint(x, pltpu.VMEM) for x in (state, grad)))


def solution(mesh):
    return jax.shard_map(
        on_device,
        mesh=mesh,
        in_specs=(
            P(None, "gx", "gy", None),
            P("gx", "gy", None),
            P("gx", "gy", None),
            P("gx", "gy", None),
            P("gx", None, "gy", None, None),
            P("gx", None, "gy", None),
            P("gx", None),
        ),
        out_specs=(P(None, "gx", "gy", None), P(None, "gx", "gy", None)),
        check_vma=False,
    )
```

```python
import functools

import jax
import jax.numpy as jnp
from jax import lax
from jax.experimental import pallas as pl
from jax.experimental.pallas import tpu as pltpu
from jax.sharding import PartitionSpec as P

MESH = pl.DeviceIdType.MESH
COURANT = 0.15
VX, VY, VZ, SXX, SYY, SZZ, SXY, SXZ, SYZ = range(9)
NX, NY, NZ = 4, 32, 512
TOP, END = 8, 40
LAST = NX
RELAYED = 2
SCALE_UNIT = 2.0**31


def rows_of(shape):
    return lax.broadcasted_iota(jnp.int32, shape, 0)


def lanes_of(shape):
    return lax.broadcasted_iota(jnp.int32, shape, 1)


def z_ahead(x):
    return jnp.where(lanes_of(x.shape) == NZ - 1, 0.0, pltpu.roll(x, NZ - 1, 1))


def z_behind(x):
    return jnp.where(lanes_of(x.shape) == 0, 0.0, pltpu.roll(x, 1, 1))


def y_ahead(x, following):
    return pltpu.roll(jnp.where(rows_of(x.shape) == 0, following, x), 7, 0)


def y_behind(x, preceding):
    return pltpu.roll(jnp.where(rows_of(x.shape) == 7, preceding, x), 1, 0)


def stress_mover(field, mat_l, mat_m, strain, stored, partial, out=None, gradients=None):
    def dyn(f, layer, start):
        return field[f, layer, pl.ds(start, 8), :]

    def move_stress(step, first_layer, stride, n, _):
        i, k = first_layer + stride * (n // (NY // 8)), n % (NY // 8)
        layer, at = i + 1, pl.multiple_of(TOP + 8 * k, 8)
        before, after = pl.multiple_of(8 * k, 8), pl.multiple_of(TOP + 8 + 8 * k, 8)
        flat = pl.ds(pl.multiple_of(8 * k, 8), 8)
        vx, vy, vz = (dyn(f, layer, at) for f in (VX, VY, VZ))
        exx = vx - dyn(VX, layer - 1, at)
        eyy = vy - y_behind(vy, dyn(VY, layer, before))
        ezz = vz - z_behind(vz)
        exy = y_ahead(vx, dyn(VX, layer, after)) - vx + dyn(VY, layer + 1, at) - vy
        exz = z_ahead(vx) - vx + dyn(VZ, layer + 1, at) - vz
        eyz = z_ahead(vy) - vy + y_ahead(vz, dyn(VZ, layer, after)) - vz
        mu = COURANT * mat_m[i, flat, :]
        both = (COURANT * mat_l[i, flat, :]) * (exx + eyy + ezz)
        moved = [dyn(f, layer, at) - (both + 2.0 * mu * e) for f, e in ((SXX, exx), (SYY, eyy), (SZZ, ezz))]
        moved += [dyn(f, layer, at) - mu * e for f, e in ((SXY, exy), (SXZ, exz), (SYZ, eyz))]
        e = (exx, eyy, ezz, exy, exz, eyz)
        if step == 0:
            for f in range(6):
                field[SXX + f, layer, pl.ds(at, 8), :] = moved[f]
                strain[f, i, flat, :] = e[f]
            return 0
        for f, value in enumerate([vx, vy, vz] + moved):
            out[f, i, flat, :] = value
        f = [stored[c, i, flat, :] for c in range(6)]
        gradients[0, i, flat, :] = partial[0, i, flat, :] + (exx + eyy + ezz) * (f[0] + f[1] + f[2])
        gradients[1, i, flat, :] = partial[1, i, flat, :] + 2.0 * (exx * f[0] + eyy * f[1] + ezz * f[2]) + exy * f[3] + exz * f[4] + eyz * f[5]
        return 0

    return move_stress


def kernel(
    count, rows_gy,
    adjoint, buoyancy, lame, shear, words, factors, order,
    field, mat_l, mat_m, stored, gradients,
    mat_b, strain, held, landed, relay,
    to_lo, to_hi, to_south, to_north, to_corner,
    from_lo, from_hi, from_south, from_north, from_corner,
    square, factor_rows, order_row, inverse_row, inverse,
    load_sem, send_sem, recv_sem, halo_send, halo_recv, relay_send, relay_recv, ready,
):
    me, row = lax.axis_index("gx"), lax.axis_index("gy")
    own_x, own_y = pl.ds(1, NX), pl.ds(TOP, NY)
    has_lo, has_hi = me > 0, me < count - 1
    has_south, has_north = row > 0, row < rows_gy - 1

    loads = [
        pltpu.make_async_copy(adjoint, field.at[:, own_x, own_y, :], load_sem.at[0]),
        pltpu.make_async_copy(buoyancy, mat_b, load_sem.at[1]),
        pltpu.make_async_copy(words, held.at[:, pl.ds(0, 24), :], load_sem.at[2]),
        pltpu.make_async_copy(factors, factor_rows, load_sem.at[3]),
        pltpu.make_async_copy(lame, mat_l, load_sem.at[4]),
        pltpu.make_async_copy(shear, mat_m, load_sem.at[5]),
        pltpu.make_async_copy(order, order_row, load_sem.at[6]),
    ]
    for load in loads:
        load.start()

    x, z, y, core = me // 16, (me // 8) % 2, (me // 2) % 4, me % 2
    at_x = [((x + d) % 4) * 16 for d in range(4)]
    at_z = [((z + d) % 2) * 8 for d in range(2)]
    at_y = [((y + d) % 4) * 2 for d in range(4)]
    at_core = [(core + d) % 2 for d in range(2)]

    def peer(dx, dz, dy, dcore):
        return at_x[dx] + at_z[dz] + at_y[dy] + at_core[dcore]

    def signal(sem, device):
        pl.semaphore_signal(sem, inc=1, device_id=device, device_id_type=MESH)

    exists = {
        (-1, 0): has_lo, (1, 0): has_hi, (0, -1): has_south, (0, 1): has_north,
        (-1, -1): has_lo & has_south, (1, 1): has_hi & has_north,
        (1, -1): has_hi & has_south, (-1, 1): has_lo & has_north,
    }

    barrier = pltpu.get_barrier_semaphore()

    along_x = [peer(d, 0, 0, 0) for d in (1, 2, 3)]
    along_y = [peer(0, 0, d, 0) for d in (1, 2, 3)]
    across_z, across_core = peer(0, 1, 0, 0), peer(0, 0, 0, 1)
    other_half = [peer(dx, 1, dy, dcore) for dcore in range(2) for dx in range(4) for dy in range(4)]
    lines = along_x + along_y + [across_core]
    for other in lines:
        signal(barrier, {"gx": other})

    @pl.when(z == 0)
    def _():
        for other in other_half:
            signal(barrier, {"gx": other})

    expected = len(lines) + len(other_half) * z
    for (dx, dy), there in exists.items():
        expected = expected + there.astype(jnp.int32)

        @pl.when(there)
        def _():
            signal(barrier, {"gx": me + dx, "gy": row + dy})

    for there, ref in ((has_lo, from_lo), (has_hi, from_hi), (has_south, from_south), (has_north, from_north)):

        @pl.when(jnp.logical_not(there))
        def _():
            ref[...] = jnp.zeros(ref.shape, jnp.float32)

    corners = ((-1, -1), (1, 1), (1, -1), (-1, 1))
    for slot, where in enumerate(corners):

        @pl.when(jnp.logical_not(exists[where]))
        def _():
            for step in range(2):
                from_corner[step, slot] = jnp.zeros((2, NZ), jnp.float32)

    def tile(f, layer, k):
        return field[f, layer, pl.ds(TOP + 8 * k, 8), :]

    nothing = jnp.zeros((8, NZ), jnp.float32)

    def stage_layers(step):
        for k in range(NY // 8):
            at = pl.ds(8 * k, 8)
            b = COURANT * mat_b[0, at, :]
            sxy, sxz, syy, syz, szz = (tile(f, 1, k) for f in (SXY, SXZ, SYY, SYZ, SZZ))
            syy_next = tile(SYY, 1, k + 1) if k < NY // 8 - 1 else nothing
            syz_prior = tile(SYZ, 1, k - 1) if k > 0 else nothing
            to_lo[step, 0, at, :] = tile(VY, 1, k) - b * (sxy + y_ahead(syy, syy_next) - syy + syz - z_behind(syz))
            to_lo[step, 1, at, :] = tile(VZ, 1, k) - b * (
                sxz + syz - y_behind(syz, syz_prior) + z_ahead(szz) - szz
            )
            to_lo[step, 2, at, :] = tile(SXX, 1, k)
            b = COURANT * mat_b[NX - 1, at, :]
            sxx, sxy, sxz = (tile(f, LAST, k) for f in (SXX, SXY, SXZ))
            sxy_prior = tile(SXY, LAST, k - 1) if k > 0 else nothing
            to_hi[step, 0, at, :] = tile(VX, LAST, k) - b * (
                sxy - y_behind(sxy, sxy_prior) - sxx + sxz - z_behind(sxz)
            )
            to_hi[step, 1, at, :] = sxy
            to_hi[step, 2, at, :] = sxz
            if step == 0:
                to_lo[0, 3, at, :] = mat_b[0, at, :]
                to_hi[0, 3, at, :] = mat_b[NX - 1, at, :]

    def stage_rows(step):
        for i in range(NX):
            layer, at = i + 1, pl.ds(0, 8)
            raw = mat_b[i, at, :]
            b = COURANT * raw
            sxx, sxy, sxz, syy, syz, szz = (tile(f, layer, 0) for f in (SXX, SXY, SXZ, SYY, SYZ, SZZ))
            sxx_next = tile(SXX, layer + 1, 0) if i < NX - 1 else nothing
            sxz_prior = tile(SXZ, layer - 1, 0) if i > 0 else nothing
            rx = tile(VX, layer, 0) - b * (sxx_next - sxx + sxy + sxz - z_behind(sxz))
            rz = tile(VZ, layer, 0) - b * (sxz - sxz_prior + syz + z_ahead(szz) - szz)
            for f, value in enumerate((rx, rz, syy, raw)[: 4 if step == 0 else 3]):
                to_south[step, pl.ds(4 * f + i, 1), :] = value[0:1]
            k, at = NY // 8 - 1, pl.ds(NY - 8, 8)
            raw = mat_b[i, at, :]
            b = COURANT * raw
            sxy, syy, syz = (tile(f, layer, k) for f in (SXY, SYY, SYZ))
            sxy_prior = tile(SXY, layer - 1, k) if i > 0 else nothing
            ry = tile(VY, layer, k) - b * (sxy - sxy_prior - syy + syz - z_behind(syz))
            for f, value in enumerate((ry, sxy, syz, raw)[: 4 if step == 0 else 3]):
                to_north[step, pl.ds(4 * f + i, 1), :] = value[7:8]
        k = NY // 8 - 1
        to_corner[step, 0, 0:1] = tile(SXY, LAST, k)[7:8]
        to_corner[step, 1, 0:1] = tile(SXX, 1, 0)[0:1]
        to_corner[step, 1, 1:2] = tile(SYY, 1, 0)[0:1]
        to_corner[step, 2, 0:1] = tile(SYZ, 1, k)[7:8]
        to_corner[step, 3, 0:1] = tile(SXZ, LAST, 0)[0:1]

    def halo_copies(step, which=slice(None)):
        full = 4 if step == 0 else 3
        faces = [
            (to_lo.at[step, pl.ds(0, full)], from_hi.at[step, pl.ds(0, full)], (-1, 0)),
            (to_hi.at[step, pl.ds(0, full)], from_lo.at[step, pl.ds(0, full)], (1, 0)),
            (to_south.at[step], from_north.at[step], (0, -1)),
            (to_north.at[step], from_south.at[step], (0, 1)),
        ]
        for slot, (dx, dy) in enumerate(corners):
            faces.append((to_corner.at[step, slot], from_corner.at[step, slot], (-dx, -dy)))
        return [
            (
                pltpu.make_async_remote_copy(
                    src_ref=src, dst_ref=dst, send_sem=halo_send.at[step, n], recv_sem=halo_recv.at[step, n],
                    device_id={"gx": me + dx, "gy": row + dy}, device_id_type=MESH,
                ),
                exists[(dx, dy)], exists[(-dx, -dy)],
            )
            for n, (src, dst, (dx, dy)) in list(enumerate(faces))[which]
        ]

    def send_halo(step, which):
        for copy, there, _ in halo_copies(step, which):

            @pl.when(there)
            def _():
                copy.start()

    def take_halo(step):
        for copy, _, comes in halo_copies(step):

            @pl.when(comes)
            def _():
                copy.wait_recv()

    def finish_halo(step):
        sxy_ll = from_corner[step, 0, 0:1]
        sxx_hh, syy_hh = from_corner[step, 1, 0:1], from_corner[step, 1, 1:2]
        syz_hl, sxz_lh = from_corner[step, 2, 0:1], from_corner[step, 3, 0:1]
        for k in range(NY // 8):
            at, framed = pl.ds(8 * k, 8), pl.ds(TOP + 8 * k, 8)
            b = COURANT * from_lo[0, 3, at, :]
            vx = from_lo[step, 0, at, :] - b * tile(SXX, 1, k)
            if k == 0:
                vx = jnp.where(rows_of(vx.shape) == 0, vx + b * sxy_ll, vx)
            field[VX, 0, framed, :] = vx
            b = COURANT * mat_b[0, at, :]
            field[VY, 1, framed, :] = tile(VY, 1, k) + b * from_lo[step, 1, at, :]
            field[VZ, 1, framed, :] = tile(VZ, 1, k) + b * from_lo[step, 2, at, :]
            b = COURANT * from_hi[0, 3, at, :]
            vy = from_hi[step, 0, at, :] + b * tile(SXY, LAST, k)
            vz = from_hi[step, 1, at, :] + b * tile(SXZ, LAST, k)
            if k == NY // 8 - 1:
                vy = jnp.where(rows_of(vy.shape) == 7, vy - b * syy_hh, vy)
            if k == 0:
                vz = jnp.where(rows_of(vz.shape) == 0, vz + b * syz_hl, vz)
            field[VY, LAST + 1, framed, :] = vy
            field[VZ, LAST + 1, framed, :] = vz
            b = COURANT * mat_b[NX - 1, at, :]
            field[VX, LAST, framed, :] = tile(VX, LAST, k) - b * from_hi[step, 2, at, :]
        first, final = pl.ds(TOP, 1), pl.ds(END - 1, 1)
        for i in range(NX):
            layer = i + 1
            part, sxy, syz = (from_south[step, pl.ds(4 * f + i, 1), :] for f in range(3))
            b = COURANT * from_south[0, pl.ds(12 + i, 1), :]
            vy = part - b * field[SYY, layer, first, :]
            if i == 0:
                vy = vy + b * sxy_ll
            field[VY, layer, pl.ds(TOP - 1, 1), :] = vy
            b = COURANT * mat_b[i, 0:1, :]
            field[VX, layer, first, :] = field[VX, layer, first, :] + b * sxy
            field[VZ, layer, first, :] = field[VZ, layer, first, :] + b * syz
            part_x, part_z, syy = (from_north[step, pl.ds(4 * f + i, 1), :] for f in range(3))
            b = COURANT * from_north[0, pl.ds(12 + i, 1), :]
            vx = part_x + b * field[SXY, layer, final, :]
            vz = part_z + b * field[SYZ, layer, final, :]
            if i == NX - 1:
                vx = vx - b * sxx_hh
            if i == 0:
                vz = vz + b * sxz_lh
            field[VX, layer, pl.ds(END, 1), :] = vx
            field[VZ, layer, pl.ds(END, 1), :] = vz
            b = COURANT * mat_b[i, NY - 1 : NY, :]
            field[VY, layer, final, :] = field[VY, layer, final, :] - b * syy

    def dyn(f, layer, start):
        return field[f, layer, pl.ds(start, 8), :]

    def move_velocity(n, _):
        i, k = n // (NY // 8), n % (NY // 8)
        layer, at = i + 1, pl.multiple_of(TOP + 8 * k, 8)
        before, after = pl.multiple_of(8 * k, 8), pl.multiple_of(TOP + 8 + 8 * k, 8)
        b = COURANT * mat_b[i, pl.ds(pl.multiple_of(8 * k, 8), 8), :]
        sxx, syy, szz, sxy, sxz, syz = (dyn(f, layer, at) for f in (SXX, SYY, SZZ, SXY, SXZ, SYZ))
        dx = dyn(SXX, layer + 1, at) - sxx + sxy - y_behind(sxy, dyn(SXY, layer, before)) + sxz - z_behind(sxz)
        field[VX, layer, pl.ds(at, 8), :] = dyn(VX, layer, at) - b * dx
        dy = sxy - dyn(SXY, layer - 1, at) + y_ahead(syy, dyn(SYY, layer, after)) - syy + syz - z_behind(syz)
        field[VY, layer, pl.ds(at, 8), :] = dyn(VY, layer, at) - b * dy
        dz = sxz - dyn(SXZ, layer - 1, at) + syz - y_behind(syz, dyn(SYZ, layer, before)) + z_ahead(szz) - szz
        field[VZ, layer, pl.ds(at, 8), :] = dyn(VZ, layer, at) - b * dz
        return 0

    move_stress = stress_mover(field, mat_l, mat_m, strain, stored, gradients)

    blank = jnp.zeros((NY, NZ), jnp.float32)
    field[SXX, LAST + 1, pl.ds(TOP, NY), :] = blank
    field[SXY, 0, pl.ds(TOP, NY), :] = blank
    field[SXZ, 0, pl.ds(TOP, NY), :] = blank
    for layer in range(1, NX + 1):
        field[SYY, layer, pl.ds(END, 8), :] = nothing
        field[SXY, layer, 0:TOP, :] = nothing
        field[SYZ, layer, 0:TOP, :] = nothing

    def prepare_blocks():
        loads[3].wait()
        loads[2].wait()
        for c in range(12):
            square[pl.ds(c, 1), 0:64] = factor_rows[c]
        turned = jnp.round(square[...].T * SCALE_UNIT).astype(jnp.int32)
        for owner in range(64):
            held[owner, 24:25, :] = turned[owner : owner + 1]
        places = jnp.broadcast_to(square[16:17, :], (128, 128)).T
        hits = places == lanes_of((128, 128)).astype(jnp.float32)
        found = jnp.sum(jnp.where(hits, rows_of((128, 128)), 0), axis=0, keepdims=True)
        inverse_row[...] = found

    loads[0].wait()
    loads[1].wait()
    stage_layers(0)
    stage_rows(0)

    def exchange(other):
        return pltpu.make_async_remote_copy(
            src_ref=held.at[other, pl.ds(0, 25)], dst_ref=landed.at[me, pl.ds(0, 25)],
            send_sem=send_sem, recv_sem=recv_sem,
            device_id={"gx": other}, device_id_type=MESH,
        )

    def blocks_of(ref, sem, number):
        some = ref.at[pl.ds(0, number), pl.ds(0, 25)]
        return pltpu.make_async_copy(some, some, sem)

    def send_near(dcore):
        for dx in range(4):
            for dy in range(4):
                if (dx, dy, dcore) != (0, 0, 0):
                    exchange(peer(dx, 0, dy, dcore)).start()

    edge = (y == 0) | (y == 3)

    def send_far(dcore):
        for dx in range(4):
            if dx == RELAYED:
                continue
            for dy in range(4):
                exchange(peer(dx, 1, dy, dcore)).start()

    def send_far_middle(dcore):
        for dy in range(4):
            exchange(peer(RELAYED, 1, dy, dcore)).start()

    def relayed_owner(n):
        return at_x[RELAYED] + at_z[1] + n

    def to_relay(n):
        owner = relayed_owner(n)
        return pltpu.make_async_remote_copy(
            src_ref=held.at[owner, pl.ds(0, 25)], dst_ref=relay.at[n, pl.ds(0, 25)],
            send_sem=send_sem, recv_sem=relay_recv,
            device_id={"gx": at_x[0] + at_z[0] + (1 + y // 3) * 2 + core}, device_id_type=MESH,
        )

    def from_relay(n):
        holder = at_x[0] + at_z[0] + (y - 1) * 3 * 2 + core
        return pltpu.make_async_remote_copy(
            src_ref=relay.at[n, pl.ds(0, 25)], dst_ref=landed.at[holder, pl.ds(0, 25)],
            send_sem=relay_send, recv_sem=recv_sem,
            device_id={"gx": relayed_owner(n)}, device_id_type=MESH,
        )

    pl.semaphore_wait(barrier, expected)
    send_halo(0, slice(None))
    for other in along_x:
        signal(ready.at[0], {"gx": other})
    square[...] = jnp.full((128, 128), 999.0, jnp.float32)
    loads[6].wait()
    square[16:17, 0:64] = order_row[...].astype(jnp.float32)
    prepare_blocks()

    @pl.when(edge)
    def _():
        for n in range(8):
            to_relay(n).start()

    @pl.when((z == 1) & jnp.logical_not(edge))
    def _():
        for dcore in range(2):
            send_far(dcore)
            send_far_middle(dcore)

    landed[me] = held[me]
    to_smem = pltpu.make_async_copy(inverse_row, inverse, load_sem.at[7])
    to_smem.start()
    pl.semaphore_wait(ready.at[0], 3)
    signal(ready.at[1], {"gx": across_core})

    @pl.when(z == 1)
    def _():
        signal(ready.at[2], {"gx": across_z})

    pl.semaphore_wait(ready.at[1], 1)

    @pl.when((z == 1) & edge)
    def _():
        send_far(0)

    @pl.when(z == 0)
    def _():
        pl.semaphore_wait(ready.at[2], 1)
        signal(ready.at[3], {"gx": across_core})
        send_far(0)
        pl.semaphore_wait(ready.at[3], 1)

    @pl.when((z == 0) & jnp.logical_not(edge))
    def _():
        send_far(1)

    @pl.when((z == 0) & jnp.logical_not(edge))
    def _():
        send_far_middle(0)
        send_far_middle(1)

    @pl.when(jnp.logical_not(edge))
    def _():
        blocks_of(relay, relay_recv, 8).wait()
        for n in range(8):
            from_relay(n).start()

    send_near(0)
    send_near(1)
    loads[4].wait()
    loads[5].wait()

    def correlate(n, _):
        i, k = n // (NY // 8), n % (NY // 8)
        flat = pl.ds(pl.multiple_of(8 * k, 8), 8)
        holders = [jnp.clip(inverse[0, i * (NY // 2) + 4 * k + r], 0, count - 1) for r in range(4)]
        pair = rows_of((8, 128)) // 2
        shift = (rows_of((8, 128)) % 2) * 16

        def gathered(line):
            parts = [jnp.broadcast_to(landed[h, pl.ds(line, 1), :], (8, 128)) for h in holders]
            low = jnp.where(pair == 0, parts[0], parts[1])
            high = jnp.where(pair == 2, parts[2], parts[3])
            return jnp.where(pair < 2, low, high)

        scale_rows = gathered(24).astype(jnp.float32) * (1.0 / SCALE_UNIT)

        def block_values(c):
            scale = jnp.broadcast_to(scale_rows[:, c : c + 1], (8, 128))
            halves = [gathered(2 * c + half) ^ jnp.int32(-2147483648) for half in range(2)]
            quarters = []
            for extra in (0, 8):
                for word in halves:
                    byte = jnp.right_shift(word, shift + extra) & 255
                    quarters.append((byte.astype(jnp.float32) - 128.0) * scale)
            return jnp.concatenate(quarters, axis=1)

        e = [strain[c, i, flat, :] for c in range(6)]
        f = [block_values(c) for c in range(6)]
        gradients[0, i, flat, :] = (e[0] + e[1] + e[2]) * (f[0] + f[1] + f[2])
        gradients[1, i, flat, :] = (
            2.0 * (e[0] * f[0] + e[1] * f[1] + e[2] * f[2]) + e[3] * f[3] + e[4] * f[4] + e[5] * f[5]
        )
        for c in range(6):
            stored[c, i, flat, :] = block_values(6 + c)
        return 0

    tiles = NX * NY // 8
    lax.fori_loop(0, tiles, move_velocity, 0, unroll=2)
    take_halo(0)

    @pl.when(edge)
    def _():
        send_far(1)

    finish_halo(0)
    lax.fori_loop(0, tiles // 2, functools.partial(move_stress, 0, 0, NX - 1), 0, unroll=2)
    stage_layers(1)
    send_halo(1, slice(0, 2))
    lax.fori_loop(0, tiles // 2, functools.partial(move_stress, 0, 1, 1), 0, unroll=2)
    stage_rows(1)
    send_halo(1, slice(2, None))
    lax.fori_loop(0, tiles, move_velocity, 0, unroll=2)
    blocks_of(landed, recv_sem, count - 1).wait()
    to_smem.wait()
    lax.fori_loop(0, tiles, correlate, 0, unroll=2)
    take_halo(1)
    finish_halo(1)
    for step in range(2):
        for copy, there, _ in halo_copies(step):

            @pl.when(there)
            def _():
                copy.wait_send()

    @pl.when(jnp.logical_not(edge))
    def _():
        blocks_of(relay, relay_send, 8).wait()

    blocks_of(held, send_sem, count - 1).wait()


def last_step(field, mat_l, mat_m, stored, partial, out, gradients, state, grad, sem):
    move_stress = stress_mover(field, mat_l, mat_m, None, stored, partial, state, grad)
    copies = []
    for i in range(NX):
        lax.fori_loop(0, NY // 8, functools.partial(move_stress, 1, i, 1), 0, unroll=2)
        copies.append(pltpu.make_async_copy(state.at[:, i], out.at[:, i], sem.at[2 * i]))
        copies.append(pltpu.make_async_copy(grad.at[:, i], gradients.at[:, i], sem.at[2 * i + 1]))
        copies[-2].start()
        copies[-1].start()
    for copy in copies:
        copy.wait()


def on_device(adjoint, buoyancy, lame_lambda, shear_mu, packed, scales, perm):
    count, rows_gy = lax.axis_size("gx"), lax.axis_size("gy")
    words = packed.reshape(count, 24, 128)
    factors = jnp.transpose(scales[0], (2, 1, 0))
    any_space, in_vmem = pl.BlockSpec(memory_space=pl.ANY), pl.BlockSpec(memory_space=pltpu.VMEM)
    f32, i32 = jnp.float32, jnp.int32
    inputs = (adjoint, buoyancy, lame_lambda, shear_mu, words, factors, perm)
    inputs = [pltpu.with_memory_space_constraint(x, pltpu.HBM) for x in inputs]
    handed = pl.pallas_call(
        functools.partial(kernel, count, rows_gy),
        out_shape=(
            pltpu.VMEM((9, NX + 2, NY + 16, NZ), f32),
            pltpu.VMEM((NX, NY, NZ), f32),
            pltpu.VMEM((NX, NY, NZ), f32),
            pltpu.VMEM((6, NX, NY, NZ), f32),
            pltpu.VMEM((2, NX, NY, NZ), f32),
        ),
        in_specs=[any_space] * 7,
        out_specs=(in_vmem,) * 5,
        scratch_shapes=[
            pltpu.VMEM((NX, NY, NZ), f32),
            pltpu.VMEM((6, NX, NY, NZ), f32),
            pltpu.VMEM((64, 32, 128), i32),
            pltpu.VMEM((64, 32, 128), i32),
            pltpu.VMEM((8, 32, 128), i32),
            pltpu.VMEM((2, 4, NY, NZ), f32),
            pltpu.VMEM((2, 4, NY, NZ), f32),
            pltpu.VMEM((2, 16, NZ), f32),
            pltpu.VMEM((2, 16, NZ), f32),
            pltpu.VMEM((2, 4, 2, NZ), f32),
            pltpu.VMEM((2, 4, NY, NZ), f32),
            pltpu.VMEM((2, 4, NY, NZ), f32),
            pltpu.VMEM((2, 16, NZ), f32),
            pltpu.VMEM((2, 16, NZ), f32),
            pltpu.VMEM((2, 4, 2, NZ), f32),
            pltpu.VMEM((128, 128), f32),
            pltpu.VMEM((12, 1, 64), f32),
            pltpu.VMEM((1, 64), i32),
            pltpu.VMEM((1, 128), i32),
            pltpu.SMEM((1, 128), i32),
            pltpu.SemaphoreType.DMA((8,)),
            pltpu.SemaphoreType.DMA,
            pltpu.SemaphoreType.DMA,
            pltpu.SemaphoreType.DMA((2, 8)),
            pltpu.SemaphoreType.DMA((2, 8)),
            pltpu.SemaphoreType.DMA,
            pltpu.SemaphoreType.DMA,
            pltpu.SemaphoreType.REGULAR((4,)),
        ],
        compiler_params=pltpu.CompilerParams(
            collective_id=0, has_side_effects=True, vmem_limit_bytes=32 * 2**20
        ),
    )(*inputs)
    return pl.pallas_call(
        last_step,
        out_shape=(
            jax.ShapeDtypeStruct((9, NX, NY, NZ), f32),
            jax.ShapeDtypeStruct((2, NX, NY, NZ), f32),
        ),
        in_specs=[in_vmem] * 5,
        out_specs=(any_space, any_space),
        scratch_shapes=[
            pltpu.VMEM((9, NX, NY, NZ), f32),
            pltpu.VMEM((2, NX, NY, NZ), f32),
            pltpu.SemaphoreType.DMA((2 * NX,)),
        ],
        compiler_params=pltpu.CompilerParams(vmem_limit_bytes=8 * 2**20),
    )(*(pltpu.with_memory_space_constraint(x, pltpu.VMEM) for x in handed))


def solution(mesh):
    return jax.shard_map(
        on_device,
        mesh=mesh,
        in_specs=(
            P(None, "gx", "gy", None),
            P("gx", "gy", None),
            P("gx", "gy", None),
            P("gx", "gy", None),
            P("gx", None, "gy", None, None),
            P("gx", None, "gy", None),
            P("gx", None),
        ),
        out_specs=(P(None, "gx", "gy", None), P(None, "gx", "gy", None)),
        check_vma=False,
    )
```
